256 devices in a mesh: gx: 16 (over y_hi, x, core), gy: 8 (over z), gz: 2 (over y_lo).
Axes of the slice: x: 4, y: 4 (y_hi: 2, y_lo: 2; y = y_hi * 2 + y_lo), z: 8, core: 2. Of those that a mesh axis runs over, the one named last changes fastest.
Arguments:
- particles: float32 [32768, 512], P(('gx', 'gy', 'gz')), may hold values from -6 to 6
- scores: bfloat16 [32768, 512], P(('gx', 'gy', 'gz')), may hold values from -6 to 6
- band_power: int32 [512], replicated, may hold values from 7 to 8
Outputs:
- drift: float32 [32768, 512], P(('gx', 'gy', 'gz'))
The draws below stay inside these ranges and needn't reach their ends.
All inputs are finite; a program needn't handle non-finite values.
Results may differ from the reference program's by a relative error of at most 0.0046.
Values may be sent and summed in bfloat16 or wider, within the bound.
A program may use at most 64 MiB of HBM per device.

```python
import jax
import jax.numpy as jnp
from jax import lax

D = 512
PARTICLES = 32768


latent_dims = 16


def draw_particles(key, part):
    keys = jax.random.split(jax.random.fold_in(key, 11), 3)
    latent_scale = 0.75 ** 0.5
    basis = jax.random.normal(keys[0], (latent_dims, D), jnp.float32) / latent_dims ** 0.5
    coords = jax.random.normal(keys[1], (PARTICLES, latent_dims), jnp.float32) * latent_scale
    noise = jax.random.normal(keys[2], (PARTICLES, D), jnp.float32) * 0.5
    values = jnp.dot(coords, basis, precision=lax.Precision.HIGHEST) + noise
    return jnp.clip(values, -6.0, 6.0)


def with_ends(drawn, own_key, smallest, largest):
    shape = drawn.shape
    index_at = [jax.random.randint(jax.random.fold_in(own_key, axis), (), 0, shape[axis]) for axis in range(len(shape))]
    drawn = drawn.at[tuple(index_at)].set(smallest)
    longest = shape.index(max(shape))
    index_at[longest] = (index_at[longest] + 1) % shape[longest]
    return drawn.at[tuple(index_at)].set(largest)


def level_of(stream_key, dims, cuts, least, largest):
    loudness = 1.0
    for dim, parts in cuts:
        draws = jax.random.uniform(jax.random.fold_in(jax.random.fold_in(stream_key, 6), dim), (parts,), jnp.float32, least / len(cuts), largest / len(cuts))
        loudness = loudness * jnp.repeat(jnp.exp(draws), dims[dim] // parts).reshape((-1,) + (1,) * (len(dims) - 1 - dim))
    return loudness


def gaussian(stream_key, extent, scale, limit, shards=(), dtype=jnp.bfloat16):
    values = scale * jax.random.normal(stream_key, extent, jnp.float32)
    if shards:
        values = values * level_of(stream_key, extent, shards, -0.22, 0.18)
    return jnp.clip(values, -limit, limit).astype(dtype)


def setup_inputs(seed: int = 0) -> dict:
    key_of = jax.random.split(jax.random.key(seed), 4)
    return {
        "particles": draw_particles(jax.random.fold_in(key_of[3], 71), 0),
        "scores": gaussian(key_of[1], (PARTICLES, D), 1.0, 6.0, ((0, 256),)),
        "band_power": with_ends(jax.random.randint(key_of[2], (D,), 7, 9), jax.random.fold_in(key_of[2], 1), 7, 8).astype(jnp.int32),
    }


def kernel_terms(target_rows, sources, stacked, source_squares, weights):
    target_float = target_rows.astype(jnp.float32)
    target_squares = jnp.sum(jnp.square(target_float) * weights[None, :], axis=1)
    scaled = (target_float * weights[None, :]).astype(jnp.bfloat16)
    inner = lax.dot_general(scaled, sources, (((1,), (1,)), ((), ())), preferred_element_type=jnp.float32)
    distance = target_squares[:, None] + source_squares[None, :] - 2.0 * inner
    kernel = jnp.exp(-distance).astype(jnp.bfloat16)
    products = jnp.dot(kernel, stacked, preferred_element_type=jnp.float32)
    totals = jnp.sum(kernel.astype(jnp.float32), axis=1)
    width = target_rows.shape[1]
    return products[:, :width] + 2.0 * weights[None, :] * (target_float * totals[:, None] - products[:, width:])


def reference(particles, scores, band_power):
    weights = jnp.exp2(-band_power.astype(jnp.float32))
    rounded = particles.astype(jnp.bfloat16)
    source_squares = jnp.sum(jnp.square(rounded.astype(jnp.float32)) * weights[None, :], axis=1)
    stacked = jnp.concatenate([scores, rounded], axis=1)
    total_rows = rounded.shape[0]
    block_rows = 512 if total_rows % 512 == 0 else total_rows
    target_blocks = rounded.reshape(total_rows // block_rows, block_rows, rounded.shape[1])

    def one_block(target_rows):
        return kernel_terms(target_rows, rounded, stacked, source_squares, weights)

    drift = lax.map(one_block, target_blocks)
    return drift.reshape(total_rows, rounded.shape[1])
```

```python
import functools

import jax
import jax.numpy as jnp
from jax import lax
from jax.experimental import pallas as pl
from jax.experimental.pallas import tpu as pltpu
from jax.sharding import PartitionSpec as P

F32 = jnp.float32
BF16 = jnp.bfloat16
LOG2E = 1.4426950408889634
ROWS = 128
D = 512
GROUPS = 1
W = D // GROUPS
HALF = ROWS // 2
QUARTER = ROWS // 4
TILE = 4 * HALF
COPIES = 400


def neighbours():
    gx, gy, gz = lax.axis_index("gx"), lax.axis_index("gy"), lax.axis_index("gz")
    y_hi, x, core = gx // 8, (gx // 2) % 4, gx % 2
    y = y_hi * 2 + gz

    def at(x, y, z, core):
        return {"gx": (y // 2) * 8 + x * 2 + core, "gy": z, "gz": y % 2}

    ids = {"core": at(x, y, gy, 1 - core)}
    for step in (1, -1):
        ids["x", step] = at((x + step + 4) % 4, y, gy, core)
        ids["y", step] = at(x, (y + step + 4) % 4, gy, core)
        ids["z", step] = at(x, y, (gy + step + 8) % 8, core)
    return ids


def kernel(
    particles_hbm, scores_hbm, power_ref, out_ref,
    particles, scores, targets, sources, source_scores, kernels, acc,
    target_squares, source_squares, totals, inverse,
    sent, relay, arrived, sent2, relay2, arrived2,
    load_sem, send_sem, recv_sem,
):
    loads = [
        pltpu.make_async_copy(particles_hbm, particles, load_sem.at[0]),
        pltpu.make_async_copy(scores_hbm, scores, load_sem.at[1]),
    ]
    for load in loads:
        load.start()
    ids = neighbours()
    barrier = pltpu.get_barrier_semaphore()
    for device in ids.values():
        pl.semaphore_signal(barrier, inc=1, device_id=device, device_id_type=pl.DeviceIdType.MESH)

    copies = {}

    def copy(name, src, dst, device):
        n = len(copies)
        made = pltpu.make_async_remote_copy(
            src_ref=src, dst_ref=dst, send_sem=send_sem.at[n], recv_sem=recv_sem.at[n],
            device_id=ids[device], device_id_type=pl.DeviceIdType.MESH,
        )
        assert name not in copies
        copies[name] = made
        made.start()

    def arrive(name):
        copies[name].wait_recv()

    weights = jnp.exp2(-power_ref[...].astype(F32))
    for load in loads:
        load.wait()
    rounded = particles[...].astype(BF16)
    rounded_f = rounded.astype(F32)
    double = rounded_f * (2.0 * weights)
    targets[0, 0, 0:HALF] = rounded[:HALF]
    targets[1, 0, 0:HALF] = rounded[HALF:]
    sources[0, 0] = double.T.astype(BF16)
    folded = (scores[...].astype(F32) - double).astype(BF16)
    for g in range(GROUPS):
        source_scores[g, 0, 0:ROWS] = folded[:, g * W : (g + 1) * W]
    inverse[...] = jnp.broadcast_to(0.25 / weights, (ROWS, D)).T

    pl.semaphore_wait(barrier, len(ids))

    def slot(step, h):
        return h if step == 1 else 8 - h

    def z_rows(h_next, step, size):
        if h_next < 4:
            return pl.ds(0, size)
        return pl.ds(0, size // 2) if step == 1 else pl.ds(size // 2, size // 2)

    def z_send(kind, h):
        for step in (1, -1):
            src, dst = slot(step, h) % 8, slot(step, h + 1)
            if kind == "r":
                rows = z_rows(h + 1, step, D)
                a, b = sources.at[src, 0, rows], sources.at[dst, 0, rows]
            else:
                rows = z_rows(h + 1, step, ROWS)
                a, b = source_scores.at[kind, src, rows], source_scores.at[kind, dst, rows]
            copy(("z", kind, h + 1, step), a, b, ("z", step))

    def z_arrive(kind, h):
        for step in (1, -1):
            arrive(("z", kind, h, step))

    def to_core(kind, s):
        if kind == "r":
            copy(("core", kind, s), sources.at[s, 0], sources.at[s, 1], "core")
        else:
            copy(
                ("core", kind, s),
                source_scores.at[kind, s, pl.ds(0, ROWS)],
                source_scores.at[kind, s, pl.ds(ROWS, ROWS)],
                "core",
            )

    def z_step(kind, h):
        z_arrive(kind, h)
        if h < 4:
            z_send(kind, h)
        for s in {h, 8 - h}:
            to_core(kind, s)

    axes = (("x", "y"), ("y", "x"))

    def t_first(half):
        for step, land in ((1, 3), (-1, 1)):
            copy(
                ("c1", half, step),
                targets.at[half, 0, pl.ds(0, HALF)],
                targets.at[half, 0, pl.ds(land * HALF, HALF)],
                (axes[half][0], step),
            )

    def t_first_relay(half):
        for step, src, part in ((1, 3, 0), (-1, 1, QUARTER)):
            copy(
                ("c2", half, step),
                targets.at[half, 0, pl.ds(src * HALF + part, QUARTER)],
                targets.at[half, 0, pl.ds(2 * HALF + part, QUARTER)],
                (axes[half][0], step),
            )

    def t_second(half, i):
        for step, land in ((1, 3), (-1, 1)):
            copy(
                ("c3", half, i, step),
                targets.at[half, 0, pl.ds(i * HALF, HALF)],
                targets.at[half, land, pl.ds(i * HALF, HALF)],
                (axes[half][1], step),
            )

    def t_second_relay(half, i):
        for step, src, part in ((1, 3, 0), (-1, 1, QUARTER)):
            copy(
                ("c6", half, i, step),
                targets.at[half, src, pl.ds(i * HALF + part, QUARTER)],
                targets.at[half, 2, pl.ds(i * HALF + part, QUARTER)],
                (axes[half][1], step),
            )

    def t_arrive(name, *at):
        for half in (0, 1):
            for step in (1, -1):
                arrive((name, half, *at, step))

    def square_targets(half, s):
        rows = targets[half, s].astype(F32)
        total = jnp.sum(rows * rows * weights, axis=1, keepdims=True) * LOG2E
        target_squares[half, s] = jnp.broadcast_to(total, (TILE, 128))

    def square_sources(s):
        for core in (0, 1):
            part = sources[s, core].astype(F32)
            total = jnp.sum(part * part * inverse[...], axis=0, keepdims=True) * LOG2E
            source_squares[s, :, core * 128 : core * 128 + 128] = total

    def make_kernels(tiles, slots):
        for half, s in tiles:
            for k in slots:
                both = jnp.concatenate([sources[k, 0], sources[k, 1]], axis=1)
                inner = jnp.dot(targets[half, s], both, preferred_element_type=F32)
                own = target_squares[half, s]
                power = inner * LOG2E - jnp.concatenate([own, own], axis=1) - source_squares[k]
                values = jnp.exp2(power).astype(BF16)
                kernels[half, s, k] = values
                values = values.astype(F32)
                pair = values[:, :128] + values[:, 128:]
                if k == 0:
                    totals[half, s] = pair
                else:
                    totals[half, s] += pair

    def product(g, half, s, slots):
        left = jnp.concatenate([kernels[half, s, k] for k in slots], axis=1)
        right = jnp.concatenate([source_scores[g, k] for k in slots], axis=0)
        return jnp.dot(left, right, preferred_element_type=F32)

    def add_products(g, tiles, slots):
        for half, s in tiles:
            if 0 in slots:
                acc[g, half, s] = product(g, half, s, slots)
            else:
                acc[g, half, s] += product(g, half, s, slots)

    def last_product(g, half, s, slots):
        row_totals = jnp.sum(totals[half, s], axis=1, keepdims=True)
        rows = targets[half, s].astype(F32)[:, g * W : (g + 1) * W]
        scale = 2.0 * weights[:, g * W : (g + 1) * W]
        result = acc[g, half, s] + product(g, half, s, slots) + rows * scale * row_totals
        acc[g, half, s] = result
        sent[g, half, s, 0:HALF] = result[2 * HALF : 3 * HALF].astype(BF16)
        sent[g, half, s, HALF : HALF + QUARTER] = result[HALF + QUARTER : 2 * HALF].astype(BF16)
        sent[g, half, s, HALF + QUARTER : TILE // 2] = result[3 * HALF : 3 * HALF + QUARTER].astype(BF16)

    def q4(n):
        return pl.ds(n * QUARTER, QUARTER)

    def first_send(g, half, s):
        axis = axes[half][0]
        base = sent.at[g, half, s]
        copy(("rel", g, half, s, 1), base.at[q4(0)], relay.at[g, half, s, q4(0)], (axis, 1))
        copy(("rel", g, half, s, -1), base.at[q4(1)], relay.at[g, half, s, q4(1)], (axis, -1))

    def first_send_plain(g, half, s):
        axis = axes[half][0]
        base = sent.at[g, half, s]
        copy(("pln", g, half, s, 1), base.at[q4(2)], arrived.at[g, half, s, q4(1)], (axis, 1))
        copy(("pln", g, half, s, -1), base.at[q4(3)], arrived.at[g, half, s, q4(2)], (axis, -1))

    def first_add(g, half, s):
        for step in (1, -1):
            arrive(("rel", g, half, s, step))
        summed = acc[g, half, s, pl.ds(HALF, QUARTER)] + relay[g, half, s, q4(0)].astype(F32)
        sent[g, half, s, q4(4)] = summed.astype(BF16)
        summed = acc[g, half, s, pl.ds(3 * HALF + QUARTER, QUARTER)] + relay[g, half, s, q4(1)].astype(F32)
        sent[g, half, s, q4(5)] = summed.astype(BF16)

    def first_send_added(g, half, s):
        axis = axes[half][0]
        base = sent.at[g, half, s]
        copy(("add", g, half, s, 1), base.at[q4(4)], arrived.at[g, half, s, q4(0)], (axis, 1))
        copy(("add", g, half, s, -1), base.at[q4(5)], arrived.at[g, half, s, q4(3)], (axis, -1))

    def first_result(g, half, s):
        for name in ("pln", "add"):
            for step in (1, -1):
                arrive((name, g, half, s, step))
        own = acc[g, half, s, pl.ds(0, HALF)]
        came = arrived[g, half, s].astype(F32)
        return own + came[:HALF] + came[HALF:]

    def second_prepare(g, half, s):
        result = first_result(g, half, s)
        if s == 2:
            sent2[g, half, pl.ds(0, HALF)] = result.astype(BF16)
        elif s == 1:
            sent2[g, half, q4(2)] = result[QUARTER:].astype(BF16)
            acc[g, half, 1, pl.ds(0, QUARTER)] = result[:QUARTER]
        elif s == 3:
            sent2[g, half, q4(3)] = result[:QUARTER].astype(BF16)
            acc[g, half, 3, pl.ds(0, QUARTER)] = result[QUARTER:]
        else:
            acc[g, half, 0, pl.ds(0, HALF)] = result

    def second_send(g, half, s):
        axis = axes[half][1]
        base = sent2.at[g, half]
        if s == 2:
            copy(("rel2", g, half, 1), base.at[q4(0)], relay2.at[g, half, q4(0)], (axis, 1))
            copy(("rel2", g, half, -1), base.at[q4(1)], relay2.at[g, half, q4(1)], (axis, -1))
        elif s == 1:
            copy(("pln2", g, half, 1), base.at[q4(2)], arrived2.at[g, half, q4(1)], (axis, 1))
        elif s == 3:
            copy(("pln2", g, half, -1), base.at[q4(3)], arrived2.at[g, half, q4(2)], (axis, -1))

    def second_add(g, half):
        for step in (1, -1):
            arrive(("rel2", g, half, step))
        summed = acc[g, half, 1, pl.ds(0, QUARTER)] + relay2[g, half, q4(0)].astype(F32)
        sent2[g, half, q4(4)] = summed.astype(BF16)
        summed = acc[g, half, 3, pl.ds(0, QUARTER)] + relay2[g, half, q4(1)].astype(F32)
        sent2[g, half, q4(5)] = summed.astype(BF16)

    def second_send_added(g, half):
        axis = axes[half][1]
        base = sent2.at[g, half]
        copy(("add2", g, half, 1), base.at[q4(4)], arrived2.at[g, half, q4(0)], (axis, 1))
        copy(("add2", g, half, -1), base.at[q4(5)], arrived2.at[g, half, q4(3)], (axis, -1))

    def second_result(g, half):
        for name in ("pln2", "add2"):
            for step in (1, -1):
                arrive((name, g, half, step))
        came = arrived2[g, half].astype(F32)
        result = acc[g, half, 0, pl.ds(0, HALF)] + came[:HALF] + came[HALF:]
        out_ref[half * HALF : half * HALF + HALF, g * W : (g + 1) * W] = result

    groups = tuple(range(GROUPS))
    near = [(0, 0), (1, 0)]
    middle = [(half, s) for s in (1, 3) for half in (0, 1)]
    far = [(0, 2), (1, 2)]
    every = near + middle + far

    z_send("r", 0)
    to_core("r", 0)
    for half in (0, 1):
        t_first(half)
    for half in (0, 1):
        t_second(half, 0)
    for g in groups:
        z_send(g, 0)
        to_core(g, 0)

    t_arrive("c1")
    for half in (0, 1):
        t_first_relay(half)
    for i in (3, 1):
        for half in (0, 1):
            t_second(half, i)
    t_arrive("c3", 0)
    for half in (0, 1):
        t_second_relay(half, 0)
    arrive(("core", "r", 0))
    square_sources(0)
    z_step("r", 1)
    t_arrive("c2")
    for half in (0, 1):
        t_second(half, 2)
    for tile in near:
        square_targets(*tile)
    make_kernels(near, (0,))
    for g in groups:
        z_step(g, 1)
    for i in (3, 1):
        t_arrive("c3", i)
        for half in (0, 1):
            t_second_relay(half, i)
    t_arrive("c3", 2)
    for half in (0, 1):
        t_second_relay(half, 2)
    for s in (1, 7):
        arrive(("core", "r", s))
        square_sources(s)
    for tile in middle:
        square_targets(*tile)
    make_kernels(middle, (0,))
    make_kernels(near, (1, 7))
    z_step("r", 2)
    make_kernels(middle, (1, 7))
    for g in groups:
        z_step(g, 2)
    for i in range(4):
        t_arrive("c6", i)
    for tile in far:
        square_targets(*tile)
    make_kernels(far, (0, 1, 7))
    for g in groups:
        for s in (0, 1, 7):
            arrive(("core", g, s))
        add_products(g, every, (0, 1, 7))
    for s in (2, 6):
        arrive(("core", "r", s))
        square_sources(s)
    make_kernels(every, (2, 6))
    z_step("r", 3)
    for g in groups:
        for s in (2, 6):
            arrive(("core", g, s))
        add_products(g, every, (2, 6))
    for s in (3, 5):
        arrive(("core", "r", s))
        square_sources(s)
    make_kernels(every, (3, 5))
    for g in groups:
        z_step(g, 3)
    z_step("r", 4)
    for g in groups:
        for s in (3, 5):
            arrive(("core", g, s))
        add_products(g, every, (3, 5))
    arrive(("core", "r", 4))
    square_sources(4)
    make_kernels(every, (4,))
    for g in groups:
        z_step(g, 4)

    order = [(half, s) for s in (2, 1, 3, 0) for half in (0, 1)]
    for g in groups:
        arrive(("core", g, 4))
        before = None
        for tile in order + [None]:
            if tile is not None:
                last_product(g, *tile, (4,))
            if before is not None:
                first_send(g, *before)
                first_send_plain(g, *before)
            before = tile
        before = None
        for tile in order + [None]:
            if tile is not None:
                first_add(g, *tile)
            if before is not None:
                first_send_added(g, *before)
            before = tile
        before = None
        for tile in order + [None]:
            if tile is not None:
                second_prepare(g, *tile)
            if before is not None:
                second_send(g, *before)
            before = tile
        for half in (0, 1):
            second_add(g, half)
        for half in (0, 1):
            second_send_added(g, half)
        for half in (0, 1):
            second_result(g, half)

    for made in copies.values():
        made.wait_send()
    assert len(copies) <= COPIES


def local(particles, scores, power):
    return pl.pallas_call(
        kernel,
        out_shape=jax.ShapeDtypeStruct((ROWS, D), F32),
        in_specs=[
            pl.BlockSpec(memory_space=pl.ANY),
            pl.BlockSpec(memory_space=pl.ANY),
            pl.BlockSpec(memory_space=pltpu.VMEM),
        ],
        out_specs=pl.BlockSpec(memory_space=pltpu.VMEM),
        scratch_shapes=[
            pltpu.VMEM((ROWS, D), F32),
            pltpu.VMEM((ROWS, D), BF16),
            pltpu.VMEM((2, 4, TILE, D), BF16),
            pltpu.VMEM((8, 2, D, ROWS), BF16),
            pltpu.VMEM((GROUPS, 8, 2 * ROWS, W), BF16),
            pltpu.VMEM((2, 4, 8, TILE, 2 * ROWS), BF16),
            pltpu.VMEM((GROUPS, 2, 4, TILE, W), F32),
            pltpu.VMEM((2, 4, TILE, 128), F32),
            pltpu.VMEM((8, 1, 2 * ROWS), F32),
            pltpu.VMEM((2, 4, TILE, 128), F32),
            pltpu.VMEM((D, ROWS), F32),
            pltpu.VMEM((GROUPS, 2, 4, 6 * QUARTER, W), BF16),
            pltpu.VMEM((GROUPS, 2, 4, 2 * QUARTER, W), BF16),
            pltpu.VMEM((GROUPS, 2, 4, 4 * QUARTER, W), BF16),
            pltpu.VMEM((GROUPS, 2, 6 * QUARTER, W), BF16),
            pltpu.VMEM((GROUPS, 2, 2 * QUARTER, W), BF16),
            pltpu.VMEM((GROUPS, 2, 4 * QUARTER, W), BF16),
            pltpu.SemaphoreType.DMA((2,)),
            pltpu.SemaphoreType.DMA((COPIES,)),
            pltpu.SemaphoreType.DMA((COPIES,)),
        ],
        compiler_params=pltpu.CompilerParams(
            collective_id=0, has_side_effects=True, vmem_limit_bytes=56 * 2**20
        ),
    )(particles, scores, power.reshape(1, D))


def solution(mesh):
    split = P(("gx", "gy", "gz"), None)
    return jax.shard_map(
        local, mesh=mesh, in_specs=(split, split, P()), out_specs=split, check_vma=False
    )
```

```python
import functools

import jax
import jax.numpy as jnp
from jax import lax
from jax.experimental import pallas as pl
from jax.experimental.pallas import tpu as pltpu
from jax.sharding import PartitionSpec as P

F32 = jnp.float32
BF16 = jnp.bfloat16
LOG2E = 1.4426950408889634
ROWS = 128
D = 512
GROUPS = 1
W = D // GROUPS
HALF = ROWS // 2
QUARTER = ROWS // 4
TILE = 4 * HALF
COPIES = 172


def neighbours():
    gx, gy, gz = lax.axis_index("gx"), lax.axis_index("gy"), lax.axis_index("gz")
    y_hi, x, core = gx // 8, (gx // 2) % 4, gx % 2
    y = y_hi * 2 + gz

    def at(x, y, z, core):
        return {"gx": (y // 2) * 8 + x * 2 + core, "gy": z, "gz": y % 2}

    ids = {"core": at(x, y, gy, 1 - core)}
    for step in (1, -1):
        ids["x", step] = at((x + step + 4) % 4, y, gy, core)
        ids["y", step] = at(x, (y + step + 4) % 4, gy, core)
        ids["z", step] = at(x, y, (gy + step + 8) % 8, core)
    return ids


def scoped_kernel(*refs):
    pl.run_scoped(
        functools.partial(kernel, *refs),
        pltpu.SemaphoreType.DMA((2,)),
        pltpu.SemaphoreType.DMA((COPIES,)),
        pltpu.SemaphoreType.DMA((COPIES,)),
    )


def kernel(
    particles_hbm, scores_hbm, power_ref, out_ref,
    particles, scores, targets, sources, source_scores, kernels, acc,
    target_squares, source_squares, totals, inverse,
    sent, relay, arrived, sent2, relay2, arrived2,
    load_sem, send_sem, recv_sem,
):
    loads = [
        pltpu.make_async_copy(particles_hbm, particles, load_sem.at[0]),
        pltpu.make_async_copy(scores_hbm, scores, load_sem.at[1]),
    ]
    for load in loads:
        load.start()
    ids = neighbours()
    barrier = pltpu.get_barrier_semaphore()
    for device in ids.values():
        pl.semaphore_signal(barrier, inc=1, device_id=device, device_id_type=pl.DeviceIdType.MESH)

    copies = {}

    def copy(name, src, dst, device):
        n = len(copies)
        made = pltpu.make_async_remote_copy(
            src_ref=src, dst_ref=dst, send_sem=send_sem.at[n], recv_sem=recv_sem.at[n],
            device_id=ids[device], device_id_type=pl.DeviceIdType.MESH,
        )
        assert name not in copies
        copies[name] = made
        made.start()

    def arrive(name):
        copies[name].wait_recv()

    weights = jnp.exp2(-power_ref[...].astype(F32))
    for load in loads:
        load.wait()
    rounded = particles[...].astype(BF16)
    rounded_f = rounded.astype(F32)
    double = rounded_f * (2.0 * weights)
    targets[0, 0, 0:HALF] = rounded[:HALF]
    targets[1, 0, 0:HALF] = rounded[HALF:]
    sources[0, 0] = double.T.astype(BF16)
    folded = (scores[...].astype(F32) - double).astype(BF16)
    for g in range(GROUPS):
        source_scores[g, 0, 0:ROWS] = folded[:, g * W : (g + 1) * W]
    inverse[...] = jnp.broadcast_to(0.25 / weights, (ROWS, D)).T

    pl.semaphore_wait(barrier, len(ids))

    def slot(step, h):
        return h if step == 1 else 8 - h

    def piece(size, step, n):
        first = 0 if step == 1 else 1
        return pl.ds((first + n) % 2 * (size // 2), size // 2)

    def z_send(kind, h, n):
        for step in (1, -1):
            src, dst = slot(step, h) % 8, slot(step, h + 1)
            if kind == "r":
                rows = piece(D, step, n)
                a, b = sources.at[src, 0, rows], sources.at[dst, 0, rows]
            else:
                rows = piece(ROWS, step, n)
                a, b = source_scores.at[kind, src, rows], source_scores.at[kind, dst, rows]
            copy(("z", kind, h + 1, n, step), a, b, ("z", step))

    def to_core(kind, s):
        if kind == "r":
            copy(("core", kind, s), sources.at[s, 0], sources.at[s, 1], "core")
        else:
            copy(
                ("core", kind, s),
                source_scores.at[kind, s, pl.ds(0, ROWS)],
                source_scores.at[kind, s, pl.ds(ROWS, ROWS)],
                "core",
            )

    def z_step(kind, h, n):
        for step in (1, -1):
            arrive(("z", kind, h, n, step))
        if h < 3 or (h == 3 and n == 0):
            z_send(kind, h, n)
        if n == 1 or h == 4:
            for s in sorted({h, 8 - h}):
                to_core(kind, s)

    axes = (("x", "y"), ("y", "x"))

    def t_first(half):
        for step, land in ((1, 3), (-1, 1)):
            copy(
                ("c1", half, step),
                targets.at[half, 0, pl.ds(0, HALF)],
                targets.at[half, 0, pl.ds(land * HALF, HALF)],
                (axes[half][0], step),
            )

    def t_first_relay(half):
        for step, src, part in ((1, 3, 0), (-1, 1, QUARTER)):
            copy(
                ("c2", half, step),
                targets.at[half, 0, pl.ds(src * HALF + part, QUARTER)],
                targets.at[half, 0, pl.ds(2 * HALF + part, QUARTER)],
                (axes[half][0], step),
            )

    def t_second(half, i):
        for step, land in ((1, 3), (-1, 1)):
            copy(
                ("c3", half, i, step),
                targets.at[half, 0, pl.ds(i * HALF, HALF)],
                targets.at[half, land, pl.ds(i * HALF, HALF)],
                (axes[half][1], step),
            )

    def t_second_relay(half, i):
        for step, src, part in ((1, 3, 0), (-1, 1, QUARTER)):
            copy(
                ("c6", half, i, step),
                targets.at[half, src, pl.ds(i * HALF + part, QUARTER)],
                targets.at[half, 2, pl.ds(i * HALF + part, QUARTER)],
                (axes[half][1], step),
            )

    def t_arrive(name, *at):
        for half in (0, 1):
            for step in (1, -1):
                arrive((name, half, *at, step))

    def square_targets(half, s):
        rows = targets[half, s].astype(F32)
        total = jnp.sum(rows * rows * weights, axis=1, keepdims=True) * LOG2E
        target_squares[half, s] = jnp.broadcast_to(total, (TILE, 128))

    def square_sources(s):
        for core in (0, 1):
            part = sources[s, core].astype(F32)
            total = jnp.sum(part * part * inverse[...], axis=0, keepdims=True) * LOG2E
            source_squares[s, :, core * 128 : core * 128 + 128] = total

    def make_kernels(tiles, slots):
        for half, s in tiles:
            for k in slots:
                both = jnp.concatenate([sources[k, 0], sources[k, 1]], axis=1)
                inner = jnp.dot(targets[half, s], both, preferred_element_type=F32)
                own = target_squares[half, s]
                power = inner * LOG2E - jnp.concatenate([own, own], axis=1) - source_squares[k]
                values = jnp.exp2(power).astype(BF16)
                kernels[half, s, k] = values
                values = values.astype(F32)
                pair = values[:, :128] + values[:, 128:]
                if k == 0:
                    totals[half, s] = pair
                else:
                    totals[half, s] += pair

    def product(g, half, s, slots):
        left = jnp.concatenate([kernels[half, s, k] for k in slots], axis=1)
        right = jnp.concatenate([source_scores[g, k] for k in slots], axis=0)
        return jnp.dot(left, right, preferred_element_type=F32)

    def add_products(g, tiles, slots):
        for half, s in tiles:
            if 0 in slots:
                acc[g, half, s] = product(g, half, s, slots)
            else:
                acc[g, half, s] += product(g, half, s, slots)

    def last_product(g, half, s, slots):
        row_totals = jnp.sum(totals[half, s], axis=1, keepdims=True)
        rows = targets[half, s].astype(F32)[:, g * W : (g + 1) * W]
        scale = 2.0 * weights[:, g * W : (g + 1) * W]
        result = acc[g, half, s] + product(g, half, s, slots) + rows * scale * row_totals
        acc[g, half, s] = result
        sent[g, half, s, 0:HALF] = result[2 * HALF : 3 * HALF].astype(BF16)
        sent[g, half, s, HALF : HALF + QUARTER] = result[HALF + QUARTER : 2 * HALF].astype(BF16)
        sent[g, half, s, HALF + QUARTER : TILE // 2] = result[3 * HALF : 3 * HALF + QUARTER].astype(BF16)

    def q4(n):
        return pl.ds(n * QUARTER, QUARTER)

    def first_send(g, half, s):
        axis = axes[half][0]
        base = sent.at[g, half, s]
        copy(("rel", g, half, s, 1), base.at[q4(0)], relay.at[g, half, s, q4(0)], (axis, 1))
        copy(("rel", g, half, s, -1), base.at[q4(1)], relay.at[g, half, s, q4(1)], (axis, -1))

    def first_send_plain(g, half, s):
        axis = axes[half][0]
        base = sent.at[g, half, s]
        copy(("pln", g, half, s, 1), base.at[q4(2)], arrived.at[g, half, s, q4(1)], (axis, 1))
        copy(("pln", g, half, s, -1), base.at[q4(3)], arrived.at[g, half, s, q4(2)], (axis, -1))

    def first_add(g, half, s):
        for step in (1, -1):
            arrive(("rel", g, half, s, step))
        summed = acc[g, half, s, pl.ds(HALF, QUARTER)] + relay[g, half, s, q4(0)].astype(F32)
        sent[g, half, s, q4(4)] = summed.astype(BF16)
        summed = acc[g, half, s, pl.ds(3 * HALF + QUARTER, QUARTER)] + relay[g, half, s, q4(1)].astype(F32)
        sent[g, half, s, q4(5)] = summed.astype(BF16)

    def first_send_added(g, half, s):
        axis = axes[half][0]
        base = sent.at[g, half, s]
        copy(("add", g, half, s, 1), base.at[q4(4)], arrived.at[g, half, s, q4(0)], (axis, 1))
        copy(("add", g, half, s, -1), base.at[q4(5)], arrived.at[g, half, s, q4(3)], (axis, -1))

    def first_result(g, half, s):
        for name in ("pln", "add"):
            for step in (1, -1):
                arrive((name, g, half, s, step))
        own = acc[g, half, s, pl.ds(0, HALF)]
        came = arrived[g, half, s].astype(F32)
        return own + came[:HALF] + came[HALF:]

    def second_prepare(g, half, s):
        result = first_result(g, half, s)
        if s == 2:
            sent2[g, half, pl.ds(0, HALF)] = result.astype(BF16)
        elif s == 1:
            sent2[g, half, q4(2)] = result[QUARTER:].astype(BF16)
            acc[g, half, 1, pl.ds(0, QUARTER)] = result[:QUARTER]
        elif s == 3:
            sent2[g, half, q4(3)] = result[:QUARTER].astype(BF16)
            acc[g, half, 3, pl.ds(0, QUARTER)] = result[QUARTER:]
        else:
            acc[g, half, 0, pl.ds(0, HALF)] = result

    def second_send(g, half, s):
        axis = axes[half][1]
        base = sent2.at[g, half]
        if s == 2:
            copy(("rel2", g, half, 1), base.at[q4(0)], relay2.at[g, half, q4(0)], (axis, 1))
            copy(("rel2", g, half, -1), base.at[q4(1)], relay2.at[g, half, q4(1)], (axis, -1))
        elif s == 1:
            copy(("pln2", g, half, 1), base.at[q4(2)], arrived2.at[g, half, q4(1)], (axis, 1))
        elif s == 3:
            copy(("pln2", g, half, -1), base.at[q4(3)], arrived2.at[g, half, q4(2)], (axis, -1))

    def second_add(g, half):
        for step in (1, -1):
            arrive(("rel2", g, half, step))
        summed = acc[g, half, 1, pl.ds(0, QUARTER)] + relay2[g, half, q4(0)].astype(F32)
        sent2[g, half, q4(4)] = summed.astype(BF16)
        summed = acc[g, half, 3, pl.ds(0, QUARTER)] + relay2[g, half, q4(1)].astype(F32)
        sent2[g, half, q4(5)] = summed.astype(BF16)

    def second_send_added(g, half):
        axis = axes[half][1]
        base = sent2.at[g, half]
        copy(("add2", g, half, 1), base.at[q4(4)], arrived2.at[g, half, q4(0)], (axis, 1))
        copy(("add2", g, half, -1), base.at[q4(5)], arrived2.at[g, half, q4(3)], (axis, -1))

    def second_result(g, half):
        for name in ("pln2", "add2"):
            for step in (1, -1):
                arrive((name, g, half, step))
        came = arrived2[g, half].astype(F32)
        result = acc[g, half, 0, pl.ds(0, HALF)] + came[:HALF] + came[HALF:]
        out_ref[half * HALF : half * HALF + HALF, g * W : (g + 1) * W] = result

    near = [(0, 0), (1, 0)]
    middle = [(half, s) for s in (1, 3) for half in (0, 1)]
    far = [(0, 2), (1, 2)]
    every = near + middle + far
    both = (0, 1)

    def from_core(kind, slots):
        for s in slots:
            arrive(("core", kind, s))

    def start():
        z_send("r", 0, 0)
        for half in both:
            t_first(half)
        for half in both:
            t_second(half, 0)
        z_send("r", 0, 1)
        to_core("r", 0)
        z_send(0, 0, 0)
        z_send(0, 0, 1)
        to_core(0, 0)

    def t_step1():
        t_arrive("c1")
        for half in both:
            t_first_relay(half)
        for i in (3, 1):
            for half in both:
                t_second(half, i)

    def t_step2():
        t_arrive("c2")
        for half in both:
            t_second(half, 2)
        t_arrive("c3", 0)
        for half in both:
            t_second_relay(half, 0)

    def t_step3(i):
        t_arrive("c3", i)
        for half in both:
            t_second_relay(half, i)

    def t_step4():
        for i in range(4):
            t_arrive("c6", i)

    start()
    t_step1()
    z_step("r", 1, 0)
    z_step("r", 1, 1)
    from_core("r", (0,))
    square_sources(0)
    z_step(0, 1, 0)
    t_step2()
    for tile in near:
        square_targets(*tile)
    make_kernels(near, (0,))
    z_step(0, 1, 1)
    t_step3(3)
    from_core("r", (1, 7))
    square_sources(1)
    square_sources(7)
    z_step("r", 2, 0)
    t_step3(1)
    make_kernels(near, (1, 7))
    z_step("r", 2, 1)
    t_step3(2)
    for tile in middle:
        square_targets(*tile)
    make_kernels(middle, (0,))
    z_step(0, 2, 0)
    make_kernels(middle, (1, 7))
    z_step(0, 2, 1)
    t_step4()
    for tile in far:
        square_targets(*tile)
    make_kernels(far, (0, 1, 7))
    z_step("r", 3, 0)
    from_core(0, (0, 1, 7))
    add_products(0, every, (0, 1, 7))
    z_step("r", 3, 1)
    from_core("r", (2, 6))
    square_sources(2)
    square_sources(6)
    make_kernels(every, (2, 6))
    z_step(0, 3, 0)
    from_core(0, (2, 6))
    add_products(0, every, (2, 6))
    from_core("r", (3, 5))
    square_sources(3)
    square_sources(5)
    z_step(0, 3, 1)
    make_kernels(every, (3, 5))
    z_step("r", 4, 0)
    from_core(0, (3, 5))
    add_products(0, every, (3, 5))
    z_step(0, 4, 0)
    from_core("r", (4,))
    square_sources(4)
    make_kernels(every, (4,))
    from_core(0, (4,))

    def for_both(f, *args):
        for half in both:
            f(0, half, *args)

    for s in (2, 1, 3, 0):
        for_both(last_product, s, (4,))
        for_both(first_send, s)
    for_both(first_send_plain, 2)
    for s in (2, 1, 3):
        for_both(first_add, s)
        for_both(first_send_added, s)
    for_both(first_send_plain, 1)
    for_both(first_send_plain, 3)
    for_both(first_add, 0)
    for_both(second_prepare, 2)
    for_both(second_send, 2)
    for_both(first_send_added, 0)
    for_both(first_send_plain, 0)
    for s in (1, 3):
        for_both(second_prepare, s)
        for_both(second_send, s)
    for_both(second_add)
    for_both(second_send_added)
    for_both(second_prepare, 0)
    for_both(second_result)

    for made in copies.values():
        made.wait_send()
    assert len(copies) <= COPIES


def local(particles, scores, power):
    return pl.pallas_call(
        scoped_kernel,
        out_shape=jax.ShapeDtypeStruct((ROWS, D), F32),
        in_specs=[
            pl.BlockSpec(memory_space=pl.ANY),
            pl.BlockSpec(memory_space=pl.ANY),
            pl.BlockSpec(memory_space=pltpu.VMEM),
        ],
        out_specs=pl.BlockSpec(memory_space=pltpu.VMEM),
        scratch_shapes=[
            pltpu.VMEM((ROWS, D), F32),
            pltpu.VMEM((ROWS, D), BF16),
            pltpu.VMEM((2, 4, TILE, D), BF16),
            pltpu.VMEM((8, 2, D, ROWS), BF16),
            pltpu.VMEM((GROUPS, 8, 2 * ROWS, W), BF16),
            pltpu.VMEM((2, 4, 8, TILE, 2 * ROWS), BF16),
            pltpu.VMEM((GROUPS, 2, 4, TILE, W), F32),
            pltpu.VMEM((2, 4, TILE, 128), F32),
            pltpu.VMEM((8, 1, 2 * ROWS), F32),
            pltpu.VMEM((2, 4, TILE, 128), F32),
            pltpu.VMEM((D, ROWS), F32),
            pltpu.VMEM((GROUPS, 2, 4, 6 * QUARTER, W), BF16),
            pltpu.VMEM((GROUPS, 2, 4, 2 * QUARTER, W), BF16),
            pltpu.VMEM((GROUPS, 2, 4, 4 * QUARTER, W), BF16),
            pltpu.VMEM((GROUPS, 2, 6 * QUARTER, W), BF16),
            pltpu.VMEM((GROUPS, 2, 2 * QUARTER, W), BF16),
            pltpu.VMEM((GROUPS, 2, 4 * QUARTER, W), BF16),
        ],
        compiler_params=pltpu.CompilerParams(
            collective_id=0, has_side_effects=True, vmem_limit_bytes=56 * 2**20
        ),
    )(particles, scores, power.reshape(1, D))


def solution(mesh):
    split = P(("gx", "gy", "gz"), None)
    return jax.shard_map(
        local, mesh=mesh, in_specs=(split, split, P()), out_specs=split, check_vma=False
    )
```

```python
import functools

import jax
import jax.numpy as jnp
from jax import lax
from jax.experimental import pallas as pl
from jax.experimental.pallas import tpu as pltpu
from jax.sharding import PartitionSpec as P

F32 = jnp.float32
BF16 = jnp.bfloat16
LOG2E = 1.4426950408889634
ROWS = 128
D = 512
GROUPS = 1
W = D // GROUPS
HALF = ROWS // 2
QUARTER = ROWS // 4
TILE = 4 * HALF
COPIES = 170


def neighbours():
    gx, gy, gz = lax.axis_index("gx"), lax.axis_index("gy"), lax.axis_index("gz")
    y_hi, x, core = gx // 8, (gx // 2) % 4, gx % 2
    y = y_hi * 2 + gz

    def at(x, y, z, core):
        return {"gx": (y // 2) * 8 + x * 2 + core, "gy": z, "gz": y % 2}

    ids = {"core": at(x, y, gy, 1 - core)}
    for step in (1, -1):
        ids["x", step] = at((x + step + 4) % 4, y, gy, core)
        ids["y", step] = at(x, (y + step + 4) % 4, gy, core)
        ids["z", step] = at(x, y, (gy + step + 8) % 8, core)
    ids["x", 2] = at((x + 2) % 4, y, gy, core)
    ids["y", 2] = at(x, (y + 2) % 4, gy, core)
    return ids


def scoped_kernel(*refs):
    pl.run_scoped(
        functools.partial(kernel, *refs),
        pltpu.SemaphoreType.DMA((3,)),
        pltpu.SemaphoreType.DMA((COPIES,)),
        pltpu.SemaphoreType.DMA((COPIES,)),
    )


def kernel(
    particles_hbm, scores_hbm, power_hbm, out_ref,
    particles, scores, power_ref, targets, sources, source_scores, kernels, acc,
    target_squares, source_squares, totals, inverse,
    sent, relay, arrived, sent2, relay2, arrived2,
    load_sem, send_sem, recv_sem,
):
    loads = [
        pltpu.make_async_copy(particles_hbm, particles, load_sem.at[0]),
        pltpu.make_async_copy(scores_hbm, scores, load_sem.at[1]),
        pltpu.make_async_copy(power_hbm, power_ref, load_sem.at[2]),
    ]
    for load in loads:
        load.start()
    ids = neighbours()
    barrier = pltpu.get_barrier_semaphore()
    for device in ids.values():
        pl.semaphore_signal(barrier, inc=1, device_id=device, device_id_type=pl.DeviceIdType.MESH)

    copies = {}

    def copy(name, src, dst, device):
        n = len(copies)
        made = pltpu.make_async_remote_copy(
            src_ref=src, dst_ref=dst, send_sem=send_sem.at[n], recv_sem=recv_sem.at[n],
            device_id=ids[device], device_id_type=pl.DeviceIdType.MESH,
        )
        assert name not in copies
        copies[name] = made
        made.start()

    def arrive(name):
        copies[name].wait_recv()

    for load in loads:
        load.wait()
    weights = jnp.exp2(-power_ref[...].astype(F32))
    rounded = particles[...].astype(BF16)
    double = rounded.astype(F32) * (2.0 * weights)
    sources[0, 0] = double.T.astype(BF16)
    targets[0, 0, 0:HALF] = rounded[:HALF]
    targets[1, 0, 0:HALF] = rounded[HALF:]
    folded = (scores[...].astype(F32) - double).astype(BF16)
    for g in range(GROUPS):
        source_scores[g, 0, 0:ROWS] = folded[:, g * W : (g + 1) * W]

    pl.semaphore_wait(barrier, len(ids))

    def slot(step, h):
        return h if step == 1 else 8 - h

    def piece(size, step, n):
        first = 0 if step == 1 else 1
        return pl.ds((first + n) % 2 * (size // 2), size // 2)

    def z_send(kind, h, n):
        for step in (1, -1):
            src, dst = slot(step, h) % 8, slot(step, h + 1)
            if kind == "r":
                rows = piece(D, step, n)
                a, b = sources.at[src, 0, rows], sources.at[dst, 0, rows]
            else:
                rows = piece(ROWS, step, n)
                a, b = source_scores.at[kind, src, rows], source_scores.at[kind, dst, rows]
            copy(("z", kind, h + 1, n, step), a, b, ("z", step))

    def to_core(kind, s):
        if kind == "r":
            copy(("core", kind, s), sources.at[s, 0], sources.at[s, 1], "core")
        else:
            copy(
                ("core", kind, s),
                source_scores.at[kind, s, pl.ds(0, ROWS)],
                source_scores.at[kind, s, pl.ds(ROWS, ROWS)],
                "core",
            )

    def z_step(kind, h, n):
        for step in (1, -1):
            arrive(("z", kind, h, n, step))
        if h < 3 or (h == 3 and n == 0):
            z_send(kind, h, n)
        if n == 1 or h == 4:
            for s in sorted({h, 8 - h}):
                to_core(kind, s)

    axes = (("x", "y"), ("y", "x"))

    def t_first(half):
        for step, land in ((1, 3), (-1, 1)):
            copy(
                ("c1", half, step),
                targets.at[half, 0, pl.ds(0, HALF)],
                targets.at[half, 0, pl.ds(land * HALF, HALF)],
                (axes[half][0], step),
            )

    def t_first_far(half):
        copy(
            ("c2", half),
            targets.at[half, 0, pl.ds(0, HALF)],
            targets.at[half, 0, pl.ds(2 * HALF, HALF)],
            (axes[half][0], 2),
        )

    def t_second(half, i):
        for step, land in ((1, 3), (-1, 1)):
            copy(
                ("c3", half, i, step),
                targets.at[half, 0, pl.ds(i * HALF, HALF)],
                targets.at[half, land, pl.ds(i * HALF, HALF)],
                (axes[half][1], step),
            )

    def t_second_relay(half, i):
        for step, src, part in ((1, 3, 0), (-1, 1, QUARTER)):
            copy(
                ("c6", half, i, step),
                targets.at[half, src, pl.ds(i * HALF + part, QUARTER)],
                targets.at[half, 2, pl.ds(i * HALF + part, QUARTER)],
                (axes[half][1], step),
            )

    def t_arrive(name, *at):
        for half in (0, 1):
            for step in (1, -1):
                arrive((name, half, *at, step))

    def square_targets(half, s):
        rows = targets[half, s].astype(F32)
        total = jnp.sum(rows * rows * weights, axis=1, keepdims=True) * LOG2E
        target_squares[half, s] = jnp.broadcast_to(total, (TILE, 128))

    def square_sources(s):
        for core in (0, 1):
            part = sources[s, core].astype(F32)
            total = jnp.sum(part * part * inverse[...], axis=0, keepdims=True) * LOG2E
            source_squares[s, :, core * 128 : core * 128 + 128] = total

    def make_kernels(tiles, slots):
        for half, s in tiles:
            for k in slots:
                both = jnp.concatenate([sources[k, 0], sources[k, 1]], axis=1)
                inner = jnp.dot(targets[half, s], both, preferred_element_type=F32)
                own = target_squares[half, s]
                power = inner * LOG2E - jnp.concatenate([own, own], axis=1) - source_squares[k]
                values = jnp.exp2(power).astype(BF16)
                kernels[half, s, k] = values
                values = values.astype(F32)
                pair = values[:, :128] + values[:, 128:]
                if k == 0:
                    totals[half, s] = pair
                else:
                    totals[half, s] += pair

    def product(g, half, s, slots):
        left = jnp.concatenate([kernels[half, s, k] for k in slots], axis=1)
        right = jnp.concatenate([source_scores[g, k] for k in slots], axis=0)
        return jnp.dot(left, right, preferred_element_type=F32)

    def add_products(g, tiles, slots):
        for half, s in tiles:
            if 0 in slots:
                acc[g, half, s] = product(g, half, s, slots)
            else:
                acc[g, half, s] += product(g, half, s, slots)

    def last_product(g, half, s, slots):
        row_totals = jnp.sum(totals[half, s], axis=1, keepdims=True)
        rows = targets[half, s].astype(F32)[:, g * W : (g + 1) * W]
        scale = 2.0 * weights[:, g * W : (g + 1) * W]
        result = acc[g, half, s] + product(g, half, s, slots) + rows * scale * row_totals
        acc[g, half, s] = result
        sent[g, half, s, 0:HALF] = result[2 * HALF : 3 * HALF].astype(BF16)
        sent[g, half, s, HALF : HALF + QUARTER] = result[HALF + QUARTER : 2 * HALF].astype(BF16)
        sent[g, half, s, HALF + QUARTER : TILE // 2] = result[3 * HALF : 3 * HALF + QUARTER].astype(BF16)

    def q4(n):
        return pl.ds(n * QUARTER, QUARTER)

    def first_send(g, half, s):
        axis = axes[half][0]
        base = sent.at[g, half, s]
        copy(("rel", g, half, s, 1), base.at[q4(0)], relay.at[g, half, s, q4(0)], (axis, 1))
        copy(("rel", g, half, s, -1), base.at[q4(1)], relay.at[g, half, s, q4(1)], (axis, -1))

    def first_send_plain(g, half, s):
        axis = axes[half][0]
        base = sent.at[g, half, s]
        copy(("pln", g, half, s, 1), base.at[q4(2)], arrived.at[g, half, s, q4(1)], (axis, 1))
        copy(("pln", g, half, s, -1), base.at[q4(3)], arrived.at[g, half, s, q4(2)], (axis, -1))

    def first_add(g, half, s):
        for step in (1, -1):
            arrive(("rel", g, half, s, step))
        summed = acc[g, half, s, pl.ds(HALF, QUARTER)] + relay[g, half, s, q4(0)].astype(F32)
        sent[g, half, s, q4(4)] = summed.astype(BF16)
        summed = acc[g, half, s, pl.ds(3 * HALF + QUARTER, QUARTER)] + relay[g, half, s, q4(1)].astype(F32)
        sent[g, half, s, q4(5)] = summed.astype(BF16)

    def first_send_added(g, half, s):
        axis = axes[half][0]
        base = sent.at[g, half, s]
        copy(("add", g, half, s, 1), base.at[q4(4)], arrived.at[g, half, s, q4(0)], (axis, 1))
        copy(("add", g, half, s, -1), base.at[q4(5)], arrived.at[g, half, s, q4(3)], (axis, -1))

    def first_result(g, half, s):
        for name in ("pln", "add"):
            for step in (1, -1):
                arrive((name, g, half, s, step))
        own = acc[g, half, s, pl.ds(0, HALF)]
        came = arrived[g, half, s].astype(F32)
        return own + came[:HALF] + came[HALF:]

    def second_prepare(g, half, s):
        result = first_result(g, half, s)
        if s == 2:
            sent2[g, half, pl.ds(0, HALF)] = result.astype(BF16)
        elif s == 1:
            sent2[g, half, q4(2)] = result[QUARTER:].astype(BF16)
            acc[g, half, 1, pl.ds(0, QUARTER)] = result[:QUARTER]
        elif s == 3:
            sent2[g, half, q4(3)] = result[:QUARTER].astype(BF16)
            acc[g, half, 3, pl.ds(0, QUARTER)] = result[QUARTER:]
        else:
            acc[g, half, 0, pl.ds(0, HALF)] = result

    def second_send(g, half, s):
        axis = axes[half][1]
        base = sent2.at[g, half]
        if s == 2:
            copy(("rel2", g, half, 1), base.at[q4(0)], relay2.at[g, half, q4(0)], (axis, 1))
            copy(("rel2", g, half, -1), base.at[q4(1)], relay2.at[g, half, q4(1)], (axis, -1))
        elif s == 1:
            copy(("pln2", g, half, 1), base.at[q4(2)], arrived2.at[g, half, q4(1)], (axis, 1))
        elif s == 3:
            copy(("pln2", g, half, -1), base.at[q4(3)], arrived2.at[g, half, q4(2)], (axis, -1))

    def second_add(g, half):
        for step in (1, -1):
            arrive(("rel2", g, half, step))
        summed = acc[g, half, 1, pl.ds(0, QUARTER)] + relay2[g, half, q4(0)].astype(F32)
        sent2[g, half, q4(4)] = summed.astype(BF16)
        summed = acc[g, half, 3, pl.ds(0, QUARTER)] + relay2[g, half, q4(1)].astype(F32)
        sent2[g, half, q4(5)] = summed.astype(BF16)

    def second_send_added(g, half):
        axis = axes[half][1]
        base = sent2.at[g, half]
        copy(("add2", g, half, 1), base.at[q4(4)], arrived2.at[g, half, q4(0)], (axis, 1))
        copy(("add2", g, half, -1), base.at[q4(5)], arrived2.at[g, half, q4(3)], (axis, -1))

    def second_result(g, half):
        for name in ("pln2", "add2"):
            for step in (1, -1):
                arrive((name, g, half, step))
        came = arrived2[g, half].astype(F32)
        result = acc[g, half, 0, pl.ds(0, HALF)] + came[:HALF] + came[HALF:]
        out_ref[half * HALF : half * HALF + HALF, g * W : (g + 1) * W] = result

    near = [(0, 0), (1, 0)]
    middle = [(half, s) for s in (1, 3) for half in (0, 1)]
    far = [(0, 2), (1, 2)]
    every = near + middle + far
    both = (0, 1)

    def from_core(kind, slots):
        for s in slots:
            arrive(("core", kind, s))

    def start():
        z_send("r", 0, 0)
        for half in both:
            t_first(half)
        for half in both:
            t_first_far(half)
        for half in both:
            t_second(half, 0)
        z_send("r", 0, 1)
        to_core("r", 0)
        z_send(0, 0, 0)
        z_send(0, 0, 1)
        to_core(0, 0)
        inverse[...] = jnp.broadcast_to(0.25 / weights, (ROWS, D)).T

    def t_step1():
        t_arrive("c1")
        for i in (3, 1):
            for half in both:
                t_second(half, i)

    def t_step2():
        for half in both:
            arrive(("c2", half))
        for half in both:
            t_second(half, 2)
        t_arrive("c3", 0)
        for half in both:
            t_second_relay(half, 0)

    def t_step3(i):
        t_arrive("c3", i)
        for half in both:
            t_second_relay(half, i)

    def t_step4():
        for i in range(4):
            t_arrive("c6", i)

    start()
    t_step1()
    z_step("r", 1, 0)
    z_step("r", 1, 1)
    from_core("r", (0,))
    square_sources(0)
    t_step2()
    z_step(0, 1, 0)
    for tile in near:
        square_targets(*tile)
    make_kernels(near, (0,))
    from_core("r", (1, 7))
    square_sources(1)
    square_sources(7)
    z_step(0, 1, 1)
    t_step3(3)
    t_step3(1)
    make_kernels(near, (1, 7))
    z_step("r", 2, 0)
    t_step3(2)
    for tile in middle:
        square_targets(*tile)
    make_kernels(middle, (0,))
    z_step("r", 2, 1)
    make_kernels(middle, (1, 7))
    z_step(0, 2, 0)
    from_core("r", (2, 6))
    square_sources(2)
    square_sources(6)
    make_kernels(near + middle, (2, 6))
    z_step(0, 2, 1)
    t_step4()
    for tile in far:
        square_targets(*tile)
    make_kernels(far, (0, 1, 7))
    z_step("r", 3, 0)
    from_core(0, (0, 1, 7))
    add_products(0, near + middle, (0, 1, 7))
    z_step("r", 3, 1)
    make_kernels(far, (2, 6))
    add_products(0, far, (0, 1, 7))
    z_step(0, 3, 0)
    from_core(0, (2, 6))
    add_products(0, every, (2, 6))
    z_step(0, 3, 1)
    from_core("r", (3, 5))
    square_sources(3)
    square_sources(5)
    make_kernels(every, (3, 5))
    z_step("r", 4, 0)
    z_step(0, 4, 0)
    from_core("r", (4,))
    square_sources(4)
    make_kernels(every, (4,))
    from_core(0, (3, 5))
    from_core(0, (4,))

    def for_both(f, *args):
        for half in both:
            f(0, half, *args)

    for s in (2, 1, 3, 0):
        for_both(last_product, s, (3, 5, 4))
        for_both(first_send, s)
    for_both(first_send_plain, 2)
    for s in (2, 1, 3):
        for_both(first_add, s)
        for_both(first_send_added, s)
    for_both(first_send_plain, 1)
    for_both(first_send_plain, 3)
    for_both(first_add, 0)
    for_both(second_prepare, 2)
    for_both(second_send, 2)
    for_both(first_send_added, 0)
    for_both(first_send_plain, 0)
    for s in (1, 3):
        for_both(second_prepare, s)
        for_both(second_send, s)
    for_both(second_add)
    for_both(second_send_added)
    for_both(second_prepare, 0)
    for_both(second_result)

    for made in copies.values():
        made.wait_send()
    assert len(copies) <= COPIES


def local(particles, scores, power):
    return pl.pallas_call(
        scoped_kernel,
        out_shape=jax.ShapeDtypeStruct((ROWS, D), F32),
        in_specs=[
            pl.BlockSpec(memory_space=pltpu.HBM),
            pl.BlockSpec(memory_space=pltpu.HBM),
            pl.BlockSpec(memory_space=pltpu.HBM),
        ],
        out_specs=pl.BlockSpec(memory_space=pltpu.VMEM),
        scratch_shapes=[
            pltpu.VMEM((ROWS, D), F32),
            pltpu.VMEM((ROWS, D), BF16),
            pltpu.VMEM((1, D), jnp.int32),
            pltpu.VMEM((2, 4, TILE, D), BF16),
            pltpu.VMEM((8, 2, D, ROWS), BF16),
            pltpu.VMEM((GROUPS, 8, 2 * ROWS, W), BF16),
            pltpu.VMEM((2, 4, 8, TILE, 2 * ROWS), BF16),
            pltpu.VMEM((GROUPS, 2, 4, TILE, W), F32),
            pltpu.VMEM((2, 4, TILE, 128), F32),
            pltpu.VMEM((8, 1, 2 * ROWS), F32),
            pltpu.VMEM((2, 4, TILE, 128), F32),
            pltpu.VMEM((D, ROWS), F32),
            pltpu.VMEM((GROUPS, 2, 4, 6 * QUARTER, W), BF16),
            pltpu.VMEM((GROUPS, 2, 4, 2 * QUARTER, W), BF16),
            pltpu.VMEM((GROUPS, 2, 4, 4 * QUARTER, W), BF16),
            pltpu.VMEM((GROUPS, 2, 6 * QUARTER, W), BF16),
            pltpu.VMEM((GROUPS, 2, 2 * QUARTER, W), BF16),
            pltpu.VMEM((GROUPS, 2, 4 * QUARTER, W), BF16),
        ],
        compiler_params=pltpu.CompilerParams(
            collective_id=0, has_side_effects=True, vmem_limit_bytes=30 * 2**20
        ),
    )(*[pltpu.with_memory_space_constraint(a, pltpu.HBM) for a in (particles, scores, power.reshape(1, D))])


def solution(mesh):
    split = P(("gx", "gy", "gz"), None)
    return jax.shard_map(
        local, mesh=mesh, in_specs=(split, split, P()), out_specs=split, check_vma=False
    )
```

```python
import functools

import jax
import jax.numpy as jnp
from jax import lax
from jax.experimental import pallas as pl
from jax.experimental.pallas import tpu as pltpu
from jax.sharding import PartitionSpec as P

F32 = jnp.float32
BF16 = jnp.bfloat16
LOG2E = 1.4426950408889634
ROWS = 128
D = 512
W = D // 2
HALF = ROWS // 2
QUARTER = ROWS // 4
TILE = 4 * HALF
COPIES = 196


def neighbours():
    gx, gy, gz = lax.axis_index("gx"), lax.axis_index("gy"), lax.axis_index("gz")
    y_hi, x, core = gx // 8, (gx // 2) % 4, gx % 2
    y = y_hi * 2 + gz

    def at(x, y, z, core):
        return {"gx": (y // 2) * 8 + x * 2 + core, "gy": z, "gz": y % 2}

    ids = {"core": at(x, y, gy, 1 - core)}
    for step in (1, -1):
        ids["x", step] = at((x + step + 4) % 4, y, gy, core)
        ids["y", step] = at(x, (y + step + 4) % 4, gy, core)
        ids["z", step] = at(x, y, (gy + step + 8) % 8, core)
    ids["x", 2] = at((x + 2) % 4, y, gy, core)
    ids["y", 2] = at(x, (y + 2) % 4, gy, core)
    ids["z", 2] = at(x, y, (gy + 2) % 8, core)
    ids["z", -2] = at(x, y, (gy + 6) % 8, core)
    return ids


def scoped_kernel(*refs):
    pl.run_scoped(
        functools.partial(kernel, *refs),
        pltpu.SemaphoreType.DMA((3,)),
        pltpu.SemaphoreType.DMA((COPIES,)),
        pltpu.SemaphoreType.DMA((COPIES,)),
    )


def kernel(
    particles_hbm, scores_hbm, power_hbm, out_ref,
    particles, scores, power_ref, targets, target_scores, sources, source_scores, kernels, acc,
    target_squares, source_squares, totals, inverse, turned,
    sent, relay, arrived, sent2, relay2, arrived2, back, gave, got, back_sent, back_came,
    load_sem, send_sem, recv_sem,
):
    loads = [
        pltpu.make_async_copy(particles_hbm, particles, load_sem.at[0]),
        pltpu.make_async_copy(scores_hbm, scores, load_sem.at[1]),
        pltpu.make_async_copy(power_hbm, power_ref, load_sem.at[2]),
    ]
    for load in loads:
        load.start()
    ids = neighbours()
    barrier = pltpu.get_barrier_semaphore()
    for device in ids.values():
        pl.semaphore_signal(barrier, inc=1, device_id=device, device_id_type=pl.DeviceIdType.MESH)

    copies = {}

    def copy(name, src, dst, device):
        n = len(copies)
        made = pltpu.make_async_remote_copy(
            src_ref=src, dst_ref=dst, send_sem=send_sem.at[n], recv_sem=recv_sem.at[n],
            device_id=ids[device], device_id_type=pl.DeviceIdType.MESH,
        )
        assert name not in copies
        copies[name] = made
        made.start()

    def arrive(name):
        copies[name].wait_recv()

    for load in loads:
        load.wait()
    weights = jnp.exp2(-power_ref[...].astype(F32))
    rounded = particles[...].astype(BF16)
    double = rounded.astype(F32) * (2.0 * weights)
    sources[0, 0] = double.T.astype(BF16)
    targets[0, 0, 0:HALF] = rounded[:HALF]
    targets[1, 0, 0:HALF] = rounded[HALF:]
    folded = (scores[...].astype(F32) - double).astype(BF16)
    source_scores[0, 0:ROWS] = folded[:, :W]
    target_scores[0, 0, 0:HALF] = folded[:HALF, W:]
    target_scores[1, 0, 0:HALF] = folded[HALF:, W:]

    pl.semaphore_wait(barrier, len(ids))

    def slot(step, h):
        return h if step == 1 else 8 - h

    def piece(size, step, n):
        first = 0 if step == 1 else 1
        return pl.ds((first + n) % 2 * (size // 2), size // 2)

    def z_send(kind, h, n):
        for step in (1, -1):
            src, dst = slot(step, h) % 8, slot(step, h + 1)
            if kind == "r":
                rows = piece(D, step, n)
                a, b = sources.at[src, 0, rows], sources.at[dst, 0, rows]
            else:
                rows = piece(ROWS, step, 0) if h == 3 else pl.ds(0, ROWS)
                a, b = source_scores.at[src, rows], source_scores.at[dst, rows]
            copy(("z", kind, h + 1, n, step), a, b, ("z", step))

    def to_core(kind, s):
        if kind == "r":
            copy(("core", kind, s), sources.at[s, 0], sources.at[s, 1], "core")
        else:
            block = source_scores.at[s]
            copy(("core", kind, s), block.at[pl.ds(0, ROWS)], block.at[pl.ds(ROWS, ROWS)], "core")

    def z_step(kind, h, n=0):
        for step in (1, -1):
            arrive(("z", kind, h, n, step))
        if h < 3 or (h == 3 and n == 0):
            z_send(kind, h, n)
        if n == 1 or h == 4 or kind == "s":
            for s in sorted({h, 8 - h}):
                to_core(kind, s)

    axes = (("x", "y"), ("y", "x"))

    def t_first(ref, half):
        for step, land in ((1, 3), (-1, 1)):
            copy(
                ("c1", ref is targets, half, step),
                ref.at[half, 0, pl.ds(0, HALF)],
                ref.at[half, 0, pl.ds(land * HALF, HALF)],
                (axes[half][0], step),
            )

    def t_first_far(ref, half):
        copy(
            ("c2", ref is targets, half),
            ref.at[half, 0, pl.ds(0, HALF)],
            ref.at[half, 0, pl.ds(2 * HALF, HALF)],
            (axes[half][0], 2),
        )

    def t_second(ref, half, i):
        for step, land in ((1, 3), (-1, 1)):
            copy(
                ("c3", ref is targets, half, i, step),
                ref.at[half, 0, pl.ds(i * HALF, HALF)],
                ref.at[half, land, pl.ds(i * HALF, HALF)],
                (axes[half][1], step),
            )

    def t_second_relay(ref, half, i):
        for step, src, part in ((1, 3, 0), (-1, 1, QUARTER)):
            copy(
                ("c6", ref is targets, half, i, step),
                ref.at[half, src, pl.ds(i * HALF + part, QUARTER)],
                ref.at[half, 2, pl.ds(i * HALF + part, QUARTER)],
                (axes[half][1], step),
            )

    def t_arrive(name, ref, *at):
        for half in (0, 1):
            for step in (1, -1):
                arrive((name, ref is targets, half, *at, step))

    def t_start(ref):
        for half in (0, 1):
            t_first(ref, half)
        for half in (0, 1):
            t_first_far(ref, half)
        for half in (0, 1):
            t_second(ref, half, 0)

    def t_step1(ref):
        t_arrive("c1", ref)
        for i in (3, 1):
            for half in (0, 1):
                t_second(ref, half, i)

    def t_step2(ref):
        for half in (0, 1):
            arrive(("c2", ref is targets, half))
        for half in (0, 1):
            t_second(ref, half, 2)
        t_arrive("c3", ref, 0)
        for half in (0, 1):
            t_second_relay(ref, half, 0)

    def t_step3(ref, i):
        t_arrive("c3", ref, i)
        for half in (0, 1):
            t_second_relay(ref, half, i)

    def t_step4(ref):
        for i in range(4):
            t_arrive("c6", ref, i)

    def square_targets(tiles):
        for half, s in tiles:
            rows = targets[half, s].astype(F32)
            total = jnp.sum(rows * rows * weights, axis=1, keepdims=True) * LOG2E
            target_squares[half, s] = jnp.broadcast_to(total, (TILE, 128))

    def square_sources(s):
        for core in (0, 1):
            part = sources[s, core].astype(F32)
            total = jnp.sum(part * part * inverse[...], axis=0, keepdims=True) * LOG2E
            source_squares[s, :, core * 128 : core * 128 + 128] = total

    def make_kernels(tiles, slots):
        for tile in tiles:
            for k in slots:
                both = jnp.concatenate([sources[k, 0], sources[k, 1]], axis=1)
                inner = jnp.dot(targets[tile], both, preferred_element_type=F32)
                own = target_squares[tile]
                power = inner * LOG2E - jnp.concatenate([own, own], axis=1) - source_squares[k]
                values = jnp.exp2(power).astype(BF16)
                kernels[(*tile, k)] = values
                values = values.astype(F32)
                pair = values[:, :128] + values[:, 128:]
                if k == 0:
                    totals[tile] = pair
                else:
                    totals[tile] += pair

    def product(half, s, slots):
        left = jnp.concatenate([kernels[half, s, k] for k in slots], axis=1)
        right = jnp.concatenate([source_scores[k] for k in slots], axis=0)
        return jnp.dot(left, right, preferred_element_type=F32)

    def last_product(half, s, slots):
        row_totals = jnp.sum(totals[half, s], axis=1, keepdims=True)
        rows = targets[half, s, :, 0:W].astype(F32)
        result = product(half, s, slots) + rows * (2.0 * weights[:, :W]) * row_totals
        acc[half, s] = result
        sent[half, s, 0:HALF] = result[2 * HALF : 3 * HALF].astype(BF16)
        sent[half, s, HALF : HALF + QUARTER] = result[HALF + QUARTER : 2 * HALF].astype(BF16)
        sent[half, s, HALF + QUARTER : TILE // 2] = result[3 * HALF : 3 * HALF + QUARTER].astype(BF16)

    def turn(tiles):
        for half, s in tiles:
            n = (half * 4 + s) * TILE
            turned[0:W, n : n + TILE] = target_scores[half, s].T

    def back_product(k):
        right = jnp.concatenate([kernels[half, s, k] for half in (0, 1) for s in range(4)], axis=0)
        rows = jnp.concatenate([sources[k, 0, W:], sources[k, 1, W:]], axis=1).astype(F32)
        result = jnp.dot(turned[...], right, preferred_element_type=F32)
        result = result[:W] + rows * result[W : W + 1]
        back[k] = result[:, :ROWS]
        gave[k] = result[:, ROWS:].astype(BF16)

    def give(k):
        copy(("give", k), gave.at[k], got.at[k], "core")

    def take(k):
        arrive(("give", k))
        back[k] += got[k].astype(F32)

    def back_rows(step, part):
        return pl.ds(part * ROWS if step == 1 else (1 - part) * ROWS, ROWS)

    def back_message(h, part):
        came = {(2, 0): ((4, 0), (3, 0)), (1, 0): ((2, 0),), (2, 1): ((3, 1),), (1, 1): ((2, 1),)}
        for n, step in enumerate((1, -1)):
            value = back[slot(step, h), back_rows(step, part)]
            for at in came.get((h, part), ()):
                arrive(("back", *at, step))
                value += back_came[(n, *at)].astype(F32)
            back_sent[n, h, part] = value.astype(BF16)

    def back_send(h, part):
        for n, step in enumerate((1, -1)):
            copy(
                ("back", h, part, step),
                back_sent.at[n, h, part],
                back_came.at[n, h, part],
                ("z", -2 * step if h == 4 else -step),
            )

    def back_result():
        for part in (0, 1):
            for n, step in enumerate((1, -1)):
                arrive(("back", 1, part, step))
                back[0, back_rows(step, part)] += back_came[n, 1, part].astype(F32)
        out_ref[:, W:] = back[0].T

    def q4(n):
        return pl.ds(n * QUARTER, QUARTER)

    def first_send(half, s):
        axis = axes[half][0]
        base = sent.at[half, s]
        copy(("rel", half, s, 1), base.at[q4(0)], relay.at[half, s, q4(0)], (axis, 1))
        copy(("rel", half, s, -1), base.at[q4(1)], relay.at[half, s, q4(1)], (axis, -1))

    def first_send_plain(half, s):
        axis = axes[half][0]
        base = sent.at[half, s]
        copy(("pln", half, s, 1), base.at[q4(2)], arrived.at[half, s, q4(1)], (axis, 1))
        copy(("pln", half, s, -1), base.at[q4(3)], arrived.at[half, s, q4(2)], (axis, -1))

    def first_add(half, s):
        for step in (1, -1):
            arrive(("rel", half, s, step))
        summed = acc[half, s, pl.ds(HALF, QUARTER)] + relay[half, s, q4(0)].astype(F32)
        sent[half, s, q4(4)] = summed.astype(BF16)
        summed = acc[half, s, pl.ds(3 * HALF + QUARTER, QUARTER)] + relay[half, s, q4(1)].astype(F32)
        sent[half, s, q4(5)] = summed.astype(BF16)

    def first_send_added(half, s):
        axis = axes[half][0]
        base = sent.at[half, s]
        copy(("add", half, s, 1), base.at[q4(4)], arrived.at[half, s, q4(0)], (axis, 1))
        copy(("add", half, s, -1), base.at[q4(5)], arrived.at[half, s, q4(3)], (axis, -1))

    def first_result(half, s):
        for name in ("pln", "add"):
            for step in (1, -1):
                arrive((name, half, s, step))
        own = acc[half, s, pl.ds(0, HALF)]
        came = arrived[half, s].astype(F32)
        return own + came[:HALF] + came[HALF:]

    def second_prepare(half, s):
        result = first_result(half, s)
        if s == 2:
            sent2[half, pl.ds(0, HALF)] = result.astype(BF16)
        elif s == 1:
            sent2[half, q4(2)] = result[QUARTER:].astype(BF16)
            acc[half, 1, pl.ds(0, QUARTER)] = result[:QUARTER]
        elif s == 3:
            sent2[half, q4(3)] = result[:QUARTER].astype(BF16)
            acc[half, 3, pl.ds(0, QUARTER)] = result[QUARTER:]
        else:
            acc[half, 0, pl.ds(0, HALF)] = result

    def second_send(half, s):
        axis = axes[half][1]
        base = sent2.at[half]
        if s == 2:
            copy(("rel2", half, 1), base.at[q4(0)], relay2.at[half, q4(0)], (axis, 1))
            copy(("rel2", half, -1), base.at[q4(1)], relay2.at[half, q4(1)], (axis, -1))
        elif s == 1:
            copy(("pln2", half, 1), base.at[q4(2)], arrived2.at[half, q4(1)], (axis, 1))
        elif s == 3:
            copy(("pln2", half, -1), base.at[q4(3)], arrived2.at[half, q4(2)], (axis, -1))

    def second_add(half):
        for step in (1, -1):
            arrive(("rel2", half, step))
        summed = acc[half, 1, pl.ds(0, QUARTER)] + relay2[half, q4(0)].astype(F32)
        sent2[half, q4(4)] = summed.astype(BF16)
        summed = acc[half, 3, pl.ds(0, QUARTER)] + relay2[half, q4(1)].astype(F32)
        sent2[half, q4(5)] = summed.astype(BF16)

    def second_send_added(half):
        axis = axes[half][1]
        base = sent2.at[half]
        copy(("add2", half, 1), base.at[q4(4)], arrived2.at[half, q4(0)], (axis, 1))
        copy(("add2", half, -1), base.at[q4(5)], arrived2.at[half, q4(3)], (axis, -1))

    def second_result(half):
        for name in ("pln2", "add2"):
            for step in (1, -1):
                arrive((name, half, step))
        came = arrived2[half].astype(F32)
        result = acc[half, 0, pl.ds(0, HALF)] + came[:HALF] + came[HALF:]
        out_ref[half * HALF : half * HALF + HALF, 0:W] = result

    near = [(0, 0), (1, 0)]
    middle = [(half, s) for s in (1, 3) for half in (0, 1)]
    far = [(0, 2), (1, 2)]
    every = near + middle + far

    def from_core(kind, slots):
        for s in slots:
            arrive(("core", kind, s))
        if kind == "r":
            for s in slots:
                square_sources(s)

    def for_both(f, *args):
        for half in (0, 1):
            f(half, *args)

    def start():
        z_send("r", 0, 0)
        t_start(targets)
        z_send("r", 0, 1)
        to_core("r", 0)
        z_send("s", 0, 0)
        to_core("s", 0)
        inverse[...] = jnp.broadcast_to(0.25 / weights, (ROWS, D)).T
        turned[W:] = jnp.ones((16, 8 * TILE), BF16)

    start()
    t_step1(targets)
    z_step("r", 1, 0)
    z_step("r", 1, 1)
    from_core("r", (0,))
    t_step2(targets)
    t_start(target_scores)
    z_step("s", 1)
    square_targets(near)
    from_core("r", (1, 7))
    make_kernels(near, (0, 1, 7))
    z_step("r", 2, 0)
    t_step3(targets, 3)
    z_step("r", 2, 1)
    t_step3(targets, 1)
    z_step("s", 2)
    t_step3(targets, 2)
    square_targets(middle)
    make_kernels(middle, (0, 1))
    z_step("r", 3, 0)
    t_step1(target_scores)
    make_kernels(middle, (7,))
    z_step("r", 3, 1)
    t_step2(target_scores)
    from_core("r", (2, 6))
    make_kernels(near + middle, (2, 6))
    z_step("s", 3)
    t_step4(targets)
    square_targets(far)
    make_kernels(far, (0, 1, 7, 2, 6))
    t_step3(target_scores, 3)
    t_step3(target_scores, 1)
    z_step("r", 4)
    from_core("r", (3, 5))
    make_kernels(every, (3, 5))
    t_step3(target_scores, 2)
    z_step("s", 4)
    from_core("r", (4,))
    from_core("s", (0, 1, 7, 2, 6, 3, 5))
    make_kernels(every, (4,))
    slots = (0, 1, 7, 2, 6, 3, 5, 4)
    from_core("s", (4,))
    for_both(last_product, 2, slots)
    t_step4(target_scores)
    for_both(first_send, 2)
    for_both(first_send_plain, 2)
    turn(every)
    for k in (4, 3, 5):
        back_product(k)
    for k in (4, 3, 5):
        give(k)
    for s in (1, 3):
        for_both(last_product, s, slots)
    for s in (1, 3):
        for_both(first_send, s)
    for k in (4, 3, 5):
        take(k)
    back_message(3, 0)
    back_message(4, 0)
    back_message(3, 1)
    for_both(first_add, 2)
    back_send(3, 0)
    back_send(4, 0)
    back_send(3, 1)
    for_both(first_send_added, 2)
    for_both(last_product, 0, slots)
    for k in (2, 6):
        back_product(k)
    give(2)
    give(6)
    for_both(first_send, 0)
    for s in (1, 3):
        for_both(first_add, s)
        for_both(first_send_added, s)
        for_both(first_send_plain, s)
    for k in (1, 7, 0):
        back_product(k)
    for k in (1, 7, 0):
        give(k)
    take(2)
    take(6)
    for_both(second_prepare, 2)
    for_both(second_send, 2)
    back_message(2, 0)
    back_message(2, 1)
    back_send(2, 0)
    back_send(2, 1)
    for_both(first_add, 0)
    for_both(first_send_added, 0)
    for_both(first_send_plain, 0)
    for k in (1, 7, 0):
        take(k)
    for s in (1, 3):
        for_both(second_prepare, s)
        for_both(second_send, s)
    for_both(second_add)
    for_both(second_send_added)
    back_message(1, 0)
    back_message(1, 1)
    back_send(1, 0)
    back_send(1, 1)
    for_both(second_prepare, 0)
    for_both(second_result)
    back_result()

    for made in copies.values():
        made.wait_send()
    assert len(copies) <= COPIES


def local(particles, scores, power):
    return pl.pallas_call(
        scoped_kernel,
        out_shape=jax.ShapeDtypeStruct((ROWS, D), F32),
        in_specs=[
            pl.BlockSpec(memory_space=pltpu.HBM),
            pl.BlockSpec(memory_space=pltpu.HBM),
            pl.BlockSpec(memory_space=pltpu.HBM),
        ],
        out_specs=pl.BlockSpec(memory_space=pltpu.VMEM),
        scratch_shapes=[
            pltpu.VMEM((ROWS, D), F32),
            pltpu.VMEM((ROWS, D), BF16),
            pltpu.VMEM((1, D), jnp.int32),
            pltpu.VMEM((2, 4, TILE, D), BF16),
            pltpu.VMEM((2, 4, TILE, W), BF16),
            pltpu.VMEM((8, 2, D, ROWS), BF16),
            pltpu.VMEM((8, 2 * ROWS, W), BF16),
            pltpu.VMEM((2, 4, 8, TILE, 2 * ROWS), BF16),
            pltpu.VMEM((2, 4, TILE, W), F32),
            pltpu.VMEM((2, 4, TILE, 128), F32),
            pltpu.VMEM((8, 1, 2 * ROWS), F32),
            pltpu.VMEM((2, 4, TILE, 128), F32),
            pltpu.VMEM((D, ROWS), F32),
            pltpu.VMEM((W + 16, 8 * TILE), BF16),
            pltpu.VMEM((2, 4, 6 * QUARTER, W), BF16),
            pltpu.VMEM((2, 4, 2 * QUARTER, W), BF16),
            pltpu.VMEM((2, 4, 4 * QUARTER, W), BF16),
            pltpu.VMEM((2, 6 * QUARTER, W), BF16),
            pltpu.VMEM((2, 2 * QUARTER, W), BF16),
            pltpu.VMEM((2, 4 * QUARTER, W), BF16),
            pltpu.VMEM((8, W, ROWS), F32),
            pltpu.VMEM((8, W, ROWS), BF16),
            pltpu.VMEM((8, W, ROWS), BF16),
            pltpu.VMEM((2, 5, 2, ROWS, ROWS), BF16),
            pltpu.VMEM((2, 5, 2, ROWS, ROWS), BF16),
        ],
        compiler_params=pltpu.CompilerParams(
            collective_id=0, has_side_effects=True, vmem_limit_bytes=30 * 2**20
        ),
    )(*[pltpu.with_memory_space_constraint(a, pltpu.HBM) for a in (particles, scores, power.reshape(1, D))])


def solution(mesh):
    split = P(("gx", "gy", "gz"), None)
    return jax.shard_map(
        local, mesh=mesh, in_specs=(split, split, P()), out_specs=split, check_vma=False
    )
```

```python
import functools

import jax
import jax.numpy as jnp
from jax import lax
from jax.experimental import pallas as pl
from jax.experimental.pallas import tpu as pltpu
from jax.sharding import PartitionSpec as P

F32 = jnp.float32
BF16 = jnp.bfloat16
LOG2E = 1.4426950408889634
ROWS = 128
D = 512
W = D // 2
HALF = ROWS // 2
QUARTER = ROWS // 4
TILE = 4 * HALF
COPIES = 192


def neighbours():
    gx, gy, gz = lax.axis_index("gx"), lax.axis_index("gy"), lax.axis_index("gz")
    y_hi, x, core = gx // 8, (gx // 2) % 4, gx % 2
    y = y_hi * 2 + gz

    def at(x, y, z, core):
        return {"gx": (y // 2) * 8 + x * 2 + core, "gy": z, "gz": y % 2}

    ids = {"core": at(x, y, gy, 1 - core)}
    for step in (1, -1):
        ids["x", step] = at((x + step + 4) % 4, y, gy, core)
        ids["y", step] = at(x, (y + step + 4) % 4, gy, core)
        ids["z", step] = at(x, y, (gy + step + 8) % 8, core)
    ids["x", 2] = at((x + 2) % 4, y, gy, core)
    ids["y", 2] = at(x, (y + 2) % 4, gy, core)
    ids["z", 2] = at(x, y, (gy + 2) % 8, core)
    ids["z", -2] = at(x, y, (gy + 6) % 8, core)
    return ids


def scoped_kernel(*refs):
    pl.run_scoped(
        functools.partial(kernel, *refs),
        pltpu.SemaphoreType.DMA((3,)),
        pltpu.SemaphoreType.DMA((COPIES,)),
        pltpu.SemaphoreType.DMA((COPIES,)),
    )


def kernel(
    particles_hbm, scores_hbm, power_hbm, out_ref,
    particles, scores, power_ref, targets, target_scores, sources, source_scores, kernels, acc,
    target_squares, source_squares, totals, inverse, turned,
    sent, relay, arrived, sent2, arrived2, back, gave, got, back_sent, back_came,
    load_sem, send_sem, recv_sem,
):
    loads = [
        pltpu.make_async_copy(particles_hbm, particles, load_sem.at[0]),
        pltpu.make_async_copy(scores_hbm, scores, load_sem.at[1]),
        pltpu.make_async_copy(power_hbm, power_ref, load_sem.at[2]),
    ]
    for load in loads:
        load.start()
    ids = neighbours()
    barrier = pltpu.get_barrier_semaphore()
    for device in ids.values():
        pl.semaphore_signal(barrier, inc=1, device_id=device, device_id_type=pl.DeviceIdType.MESH)

    copies = {}

    def copy(name, src, dst, device):
        n = len(copies)
        made = pltpu.make_async_remote_copy(
            src_ref=src, dst_ref=dst, send_sem=send_sem.at[n], recv_sem=recv_sem.at[n],
            device_id=ids[device], device_id_type=pl.DeviceIdType.MESH,
        )
        assert name not in copies
        copies[name] = made
        made.start()

    def arrive(name):
        copies[name].wait_recv()

    for load in loads:
        load.wait()
    weights = jnp.exp2(-power_ref[...].astype(F32))
    rounded = particles[...].astype(BF16)
    double = rounded.astype(F32) * (2.0 * weights)
    sources[0, 0] = double.T.astype(BF16)
    targets[0, 0, 0:HALF] = rounded[:HALF]
    targets[1, 0, 0:HALF] = rounded[HALF:]
    folded = (scores[...].astype(F32) - double).astype(BF16)
    source_scores[0, 0:ROWS] = folded[:, :W]
    target_scores[0, 0, 0:HALF] = folded[:HALF, W:]
    target_scores[1, 0, 0:HALF] = folded[HALF:, W:]

    pl.semaphore_wait(barrier, len(ids))

    def slot(step, h):
        return h if step == 1 else 8 - h

    def piece(size, step, n):
        first = 0 if step == 1 else 1
        return pl.ds((first + n) % 2 * (size // 2), size // 2)

    def z_send(kind, h, n):
        for step in (1, -1):
            src, dst = slot(step, h) % 8, slot(step, h + 1)
            if kind == "r":
                rows = piece(D, step, n)
                a, b = sources.at[src, 0, rows], sources.at[dst, 0, rows]
            else:
                rows = piece(ROWS, step, 0) if h == 3 else pl.ds(0, ROWS)
                a, b = source_scores.at[src, rows], source_scores.at[dst, rows]
            copy(("z", kind, h + 1, n, step), a, b, ("z", step))

    def to_core(kind, s):
        if kind == "r":
            copy(("core", kind, s), sources.at[s, 0], sources.at[s, 1], "core")
        else:
            block = source_scores.at[s]
            copy(("core", kind, s), block.at[pl.ds(0, ROWS)], block.at[pl.ds(ROWS, ROWS)], "core")

    def z_step(kind, h, n=0):
        for step in (1, -1):
            arrive(("z", kind, h, n, step))
        if h < 3 or (h == 3 and n == 0):
            z_send(kind, h, n)
        if n == 1 or h == 4 or kind == "s":
            for s in sorted({h, 8 - h}):
                to_core(kind, s)

    axes = (("x", "y"), ("y", "x"))

    def t_first(ref, half):
        for step, land in ((1, 3), (-1, 1)):
            copy(
                ("c1", ref is targets, half, step),
                ref.at[half, 0, pl.ds(0, HALF)],
                ref.at[half, 0, pl.ds(land * HALF, HALF)],
                (axes[half][0], step),
            )

    def t_first_far(ref, half):
        copy(
            ("c2", half),
            ref.at[half, 0, pl.ds(0, HALF)],
            ref.at[half, 0, pl.ds(2 * HALF, HALF)],
            (axes[half][0], 2),
        )

    def t_first_relay(ref, half):
        for step, src, part in ((1, 3, 0), (-1, 1, QUARTER)):
            copy(
                ("c2", half, step),
                ref.at[half, 0, pl.ds(src * HALF + part, QUARTER)],
                ref.at[half, 0, pl.ds(2 * HALF + part, QUARTER)],
                (axes[half][0], step),
            )

    def t_second(ref, half, i):
        for step, land in ((1, 3), (-1, 1)):
            copy(
                ("c3", ref is targets, half, i, step),
                ref.at[half, 0, pl.ds(i * HALF, HALF)],
                ref.at[half, land, pl.ds(i * HALF, HALF)],
                (axes[half][1], step),
            )

    def t_second_relay(ref, half, i):
        for step, src, part in ((1, 3, 0), (-1, 1, QUARTER)):
            copy(
                ("c6", ref is targets, half, i, step),
                ref.at[half, src, pl.ds(i * HALF + part, QUARTER)],
                ref.at[half, 2, pl.ds(i * HALF + part, QUARTER)],
                (axes[half][1], step),
            )

    def t_arrive(name, ref, *at):
        for half in (0, 1):
            for step in (1, -1):
                arrive((name, ref is targets, half, *at, step))

    def t_start(ref):
        for half in (0, 1):
            t_first(ref, half)
        if ref is targets:
            for half in (0, 1):
                t_first_far(ref, half)
        for half in (0, 1):
            t_second(ref, half, 0)

    def t_step1(ref):
        t_arrive("c1", ref)
        if ref is target_scores:
            for half in (0, 1):
                t_first_relay(ref, half)
        for i in (3, 1):
            for half in (0, 1):
                t_second(ref, half, i)

    def t_step2(ref):
        for half in (0, 1):
            if ref is targets:
                arrive(("c2", half))
            else:
                arrive(("c2", half, 1))
                arrive(("c2", half, -1))
        for half in (0, 1):
            t_second(ref, half, 2)

    def t_step3(ref, i):
        t_arrive("c3", ref, i)
        for half in (0, 1):
            t_second_relay(ref, half, i)

    def t_step4(ref):
        for i in range(4):
            t_arrive("c6", ref, i)

    def square_targets(tiles):
        for half, s in tiles:
            rows = targets[half, s].astype(F32)
            total = jnp.sum(rows * rows * weights, axis=1, keepdims=True) * LOG2E
            target_squares[half, s] = jnp.broadcast_to(total, (TILE, 128))

    def square_sources(s):
        for core in (0, 1):
            part = sources[s, core].astype(F32)
            total = jnp.sum(part * part * inverse[...], axis=0, keepdims=True) * LOG2E
            source_squares[s, :, core * 128 : core * 128 + 128] = total

    def make_kernels(tiles, slots):
        for tile in tiles:
            for k in slots:
                both = jnp.concatenate([sources[k, 0], sources[k, 1]], axis=1)
                inner = jnp.dot(targets[tile], both, preferred_element_type=F32)
                own = target_squares[tile]
                power = inner * LOG2E - jnp.concatenate([own, own], axis=1) - source_squares[k]
                values = jnp.exp2(power).astype(BF16)
                kernels[(*tile, k)] = values
                values = values.astype(F32)
                pair = values[:, :128] + values[:, 128:]
                if k == 0:
                    totals[tile] = pair
                else:
                    totals[tile] += pair

    def product(half, s, slots):
        left = jnp.concatenate([kernels[half, s, k] for k in slots], axis=1)
        right = jnp.concatenate([source_scores[k] for k in slots], axis=0)
        return jnp.dot(left, right, preferred_element_type=F32)

    def last_product(half, s, slots):
        row_totals = jnp.sum(totals[half, s], axis=1, keepdims=True)
        rows = targets[half, s, :, 0:W].astype(F32)
        result = product(half, s, slots) + rows * (2.0 * weights[:, :W]) * row_totals
        acc[half, s] = result
        sent[half, s, 0:HALF] = result[2 * HALF : 3 * HALF].astype(BF16)
        sent[half, s, HALF : HALF + QUARTER] = result[HALF + QUARTER : 2 * HALF].astype(BF16)
        sent[half, s, HALF + QUARTER : TILE // 2] = result[3 * HALF : 3 * HALF + QUARTER].astype(BF16)

    def turn(tiles):
        for half, s in tiles:
            n = (half * 4 + s) * TILE
            turned[0:W, n : n + TILE] = target_scores[half, s].T

    def back_product(k):
        right = jnp.concatenate([kernels[half, s, k] for half in (0, 1) for s in range(4)], axis=0)
        rows = jnp.concatenate([sources[k, 0, W:], sources[k, 1, W:]], axis=1).astype(F32)
        result = jnp.dot(turned[...], right, preferred_element_type=F32)
        result = result[:W] + rows * result[W : W + 1]
        back[k] = result[:, :ROWS]
        gave[k] = result[:, ROWS:].astype(BF16)

    def give(k):
        copy(("give", k), gave.at[k], got.at[k], "core")

    def take(k):
        arrive(("give", k))
        back[k] += got[k].astype(F32)

    def back_rows(step, part):
        return pl.ds(part * ROWS if step == 1 else (1 - part) * ROWS, ROWS)

    def back_message(h, part):
        came = ([(4, 0), (3, 0)], [(3, 1)])[part] if h == 2 else []
        for n, step in enumerate((1, -1)):
            value = back[slot(step, h), back_rows(step, part)]
            for at in came:
                arrive(("back", *at, step))
                value += back_came[(n, *at)].astype(F32)
            back_sent[n, h, part] = value.astype(BF16)

    def back_send(h, part):
        for n, step in enumerate((1, -1)):
            copy(
                ("back", h, part, step),
                back_sent.at[n, h, part],
                back_came.at[n, h, part],
                ("z", -step if h % 2 else -2 * step),
            )

    def back_result():
        for h in (1, 2):
            for part in (0, 1):
                for n, step in enumerate((1, -1)):
                    arrive(("back", h, part, step))
                    back[0, back_rows(step, part)] += back_came[n, h, part].astype(F32)
        out_ref[:, W:] = back[0].T

    def q4(n):
        return pl.ds(n * QUARTER, QUARTER)

    def first_send(half, s):
        axis = axes[half][0]
        base = sent.at[half, s]
        copy(("rel", half, s, 1), base.at[q4(0)], relay.at[half, s, q4(0)], (axis, 1))
        copy(("rel", half, s, -1), base.at[q4(1)], relay.at[half, s, q4(1)], (axis, -1))

    def first_send_plain(half, s):
        axis = axes[half][0]
        base = sent.at[half, s]
        copy(("pln", half, s, 1), base.at[q4(2)], arrived.at[half, s, q4(1)], (axis, 1))
        copy(("pln", half, s, -1), base.at[q4(3)], arrived.at[half, s, q4(2)], (axis, -1))

    def first_add(half, s):
        for step in (1, -1):
            arrive(("rel", half, s, step))
        summed = acc[half, s, pl.ds(HALF, QUARTER)] + relay[half, s, q4(0)].astype(F32)
        sent[half, s, q4(4)] = summed.astype(BF16)
        summed = acc[half, s, pl.ds(3 * HALF + QUARTER, QUARTER)] + relay[half, s, q4(1)].astype(F32)
        sent[half, s, q4(5)] = summed.astype(BF16)

    def first_send_added(half, s):
        axis = axes[half][0]
        base = sent.at[half, s]
        copy(("add", half, s, 1), base.at[q4(4)], arrived.at[half, s, q4(0)], (axis, 1))
        copy(("add", half, s, -1), base.at[q4(5)], arrived.at[half, s, q4(3)], (axis, -1))

    def first_result(half, s):
        for name in ("pln", "add"):
            for step in (1, -1):
                arrive((name, half, s, step))
        own = acc[half, s, pl.ds(0, HALF)]
        came = arrived[half, s].astype(F32)
        return own + came[:HALF] + came[HALF:]

    def second_prepare(half, s):
        result = first_result(half, s)
        if s == 0:
            acc[half, 0, pl.ds(0, HALF)] = result
        else:
            sent2[half, s - 1] = result.astype(BF16)

    def second_send(half, s):
        copy(
            ("sum2", half, s),
            sent2.at[half, s - 1],
            arrived2.at[half, s - 1],
            (axes[half][1], (1, 2, -1)[s - 1]),
        )

    def second_result(half):
        result = acc[half, 0, pl.ds(0, HALF)]
        for s in (1, 3, 2):
            arrive(("sum2", half, s))
            result += arrived2[half, s - 1].astype(F32)
        out_ref[half * HALF : half * HALF + HALF, 0:W] = result

    near = [(0, 0), (1, 0)]
    middle = [(half, s) for s in (1, 3) for half in (0, 1)]
    far = [(0, 2), (1, 2)]
    every = near + middle + far

    def from_core(kind, slots):
        for s in slots:
            arrive(("core", kind, s))
        if kind == "r":
            for s in slots:
                square_sources(s)

    def for_both(f, *args):
        for half in (0, 1):
            f(half, *args)

    def start():
        z_send("r", 0, 0)
        t_start(targets)
        z_send("r", 0, 1)
        to_core("r", 0)
        t_start(target_scores)
        z_send("s", 0, 0)
        to_core("s", 0)
        inverse[...] = jnp.broadcast_to(0.25 / weights, (ROWS, D)).T
        turned[W:] = jnp.ones((16, 8 * TILE), BF16)

    start()
    t_step1(targets)
    z_step("r", 1, 0)
    t_step2(targets)
    z_step("r", 1, 1)
    from_core("r", (0,))
    t_step3(targets, 0)
    z_step("s", 1)
    t_step1(target_scores)
    square_targets(near)
    from_core("r", (1, 7))
    make_kernels(near, (0, 1, 7))
    z_step("r", 2, 0)
    t_step3(targets, 3)
    z_step("r", 2, 1)
    t_step3(targets, 1)
    z_step("s", 2)
    t_step3(targets, 2)
    t_step3(target_scores, 0)
    square_targets(middle)
    make_kernels(middle, (0, 1))
    z_step("r", 3, 0)
    t_step2(target_scores)
    make_kernels(middle, (7,))
    z_step("r", 3, 1)
    t_step3(target_scores, 3)
    t_step3(target_scores, 1)
    from_core("r", (2, 6))
    make_kernels(near + middle, (2, 6))
    z_step("s", 3)
    t_step4(targets)
    square_targets(far)
    make_kernels(far, (0, 1, 7, 2, 6))
    z_step("r", 4)
    t_step3(target_scores, 2)
    from_core("r", (3, 5))
    make_kernels(every, (3, 5))
    z_step("s", 4)
    from_core("r", (4,))
    from_core("s", (0, 1, 7, 2, 6, 3, 5))
    make_kernels(every, (4,))
    slots = (0, 1, 7, 2, 6, 3, 5, 4)
    from_core("s", (4,))
    for_both(last_product, 2, slots)
    t_step4(target_scores)
    for_both(first_send, 2)
    for_both(first_send_plain, 2)
    turn(every)
    for k in (4, 3, 5):
        back_product(k)
    for k in (4, 3, 5):
        give(k)
    for s in (1, 3):
        for_both(last_product, s, slots)
    for k in (4, 3, 5):
        take(k)
    back_message(4, 0)
    back_message(3, 0)
    back_message(3, 1)
    for s in (1, 3):
        for_both(first_send, s)
    for_both(first_add, 2)
    back_send(4, 0)
    back_send(3, 0)
    back_send(3, 1)
    for_both(first_send_added, 2)
    for s in (1, 3):
        for_both(first_send_plain, s)
    for_both(last_product, 0, slots)
    for k in (2, 6):
        back_product(k)
    for_both(first_send, 0)
    for k in (2, 6):
        give(k)
    for k in (1, 7, 0):
        back_product(k)
    for k in (1, 7, 0):
        give(k)
    for s in (1, 3):
        for_both(first_add, s)
        for_both(first_send_added, s)
    for_both(first_send_plain, 0)
    for_both(second_prepare, 2)
    for_both(second_send, 2)
    for_both(first_add, 0)
    for_both(first_send_added, 0)
    take(2)
    take(6)
    for part in (0, 1):
        back_message(2, part)
        back_send(2, part)
    for k in (1, 7, 0):
        take(k)
    back_message(1, 0)
    back_message(1, 1)
    for s in (1, 3):
        for_both(second_prepare, s)
        for_both(second_send, s)
    back_send(1, 0)
    back_send(1, 1)
    for_both(second_prepare, 0)
    for_both(second_result)
    back_result()

    for made in copies.values():
        made.wait_send()
    assert len(copies) <= COPIES


def local(particles, scores, power):
    return pl.pallas_call(
        scoped_kernel,
        out_shape=jax.ShapeDtypeStruct((ROWS, D), F32),
        in_specs=[
            pl.BlockSpec(memory_space=pltpu.HBM),
            pl.BlockSpec(memory_space=pltpu.HBM),
            pl.BlockSpec(memory_space=pltpu.HBM),
        ],
        out_specs=pl.BlockSpec(memory_space=pltpu.VMEM),
        scratch_shapes=[
            pltpu.VMEM((ROWS, D), F32),
            pltpu.VMEM((ROWS, D), BF16),
            pltpu.VMEM((1, D), jnp.int32),
            pltpu.VMEM((2, 4, TILE, D), BF16),
            pltpu.VMEM((2, 4, TILE, W), BF16),
            pltpu.VMEM((8, 2, D, ROWS), BF16),
            pltpu.VMEM((8, 2 * ROWS, W), BF16),
            pltpu.VMEM((2, 4, 8, TILE, 2 * ROWS), BF16),
            pltpu.VMEM((2, 4, TILE, W), F32),
            pltpu.VMEM((2, 4, TILE, 128), F32),
            pltpu.VMEM((8, 1, 2 * ROWS), F32),
            pltpu.VMEM((2, 4, TILE, 128), F32),
            pltpu.VMEM((D, ROWS), F32),
            pltpu.VMEM((W + 16, 8 * TILE), BF16),
            pltpu.VMEM((2, 4, 6 * QUARTER, W), BF16),
            pltpu.VMEM((2, 4, 2 * QUARTER, W), BF16),
            pltpu.VMEM((2, 4, 4 * QUARTER, W), BF16),
            pltpu.VMEM((2, 3, HALF, W), BF16),
            pltpu.VMEM((2, 3, HALF, W), BF16),
            pltpu.VMEM((8, W, ROWS), F32),
            pltpu.VMEM((8, W, ROWS), BF16),
            pltpu.VMEM((8, W, ROWS), BF16),
            pltpu.VMEM((2, 5, 2, ROWS, ROWS), BF16),
            pltpu.VMEM((2, 5, 2, ROWS, ROWS), BF16),
        ],
        compiler_params=pltpu.CompilerParams(
            collective_id=0, has_side_effects=True, vmem_limit_bytes=30 * 2**20
        ),
    )(*[pltpu.with_memory_space_constraint(a, pltpu.HBM) for a in (particles, scores, power.reshape(1, D))])


def solution(mesh):
    split = P(("gx", "gy", "gz"), None)
    return jax.shard_map(
        local, mesh=mesh, in_specs=(split, split, P()), out_specs=split, check_vma=False
    )
```

```python
import functools

import jax
import jax.numpy as jnp
from jax import lax
from jax.experimental import pallas as pl
from jax.experimental.pallas import tpu as pltpu
from jax.sharding import PartitionSpec as P

F32 = jnp.float32
BF16 = jnp.bfloat16
LOG2E = 1.4426950408889634
ROWS = 128
D = 512
W = D // 2
HALF = ROWS // 2
QUARTER = ROWS // 4
TILE = 4 * HALF
COPIES = 186


def neighbours():
    gx, gy, gz = lax.axis_index("gx"), lax.axis_index("gy"), lax.axis_index("gz")
    y_hi, x, core = gx // 8, (gx // 2) % 4, gx % 2
    y = y_hi * 2 + gz

    def at(x, y, z, core):
        return {"gx": (y // 2) * 8 + x * 2 + core, "gy": z, "gz": y % 2}

    ids = {"core": at(x, y, gy, 1 - core)}
    for step in (1, -1):
        ids["x", step] = at((x + step + 4) % 4, y, gy, core)
        ids["y", step] = at(x, (y + step + 4) % 4, gy, core)
        ids["z", step] = at(x, y, (gy + step + 8) % 8, core)
    ids["x", 2] = at((x + 2) % 4, y, gy, core)
    ids["y", 2] = at(x, (y + 2) % 4, gy, core)
    ids["z", 2] = at(x, y, (gy + 2) % 8, core)
    ids["z", -2] = at(x, y, (gy + 6) % 8, core)
    return ids


def scoped_kernel(*refs):
    pl.run_scoped(
        functools.partial(kernel, *refs),
        pltpu.SemaphoreType.DMA((3,)),
        pltpu.SemaphoreType.DMA((COPIES,)),
        pltpu.SemaphoreType.DMA((COPIES,)),
    )


def kernel(
    particles_hbm, scores_hbm, power_hbm, out_ref,
    particles, scores, power_ref, targets, target_scores, sources, source_scores, kernels, acc,
    target_squares, source_squares, totals, inverse, turned,
    sent, relay, arrived, sent2, arrived2, back, gave, got, back_sent, back_came,
    load_sem, send_sem, recv_sem,
):
    loads = [
        pltpu.make_async_copy(particles_hbm, particles, load_sem.at[0]),
        pltpu.make_async_copy(scores_hbm, scores, load_sem.at[1]),
        pltpu.make_async_copy(power_hbm, power_ref, load_sem.at[2]),
    ]
    for load in loads:
        load.start()
    ids = neighbours()
    barrier = pltpu.get_barrier_semaphore()
    for device in ids.values():
        pl.semaphore_signal(barrier, inc=1, device_id=device, device_id_type=pl.DeviceIdType.MESH)

    copies = {}

    def copy(name, src, dst, device):
        n = len(copies)
        made = pltpu.make_async_remote_copy(
            src_ref=src, dst_ref=dst, send_sem=send_sem.at[n], recv_sem=recv_sem.at[n],
            device_id=ids[device], device_id_type=pl.DeviceIdType.MESH,
        )
        assert name not in copies
        copies[name] = made
        made.start()

    def arrive(name):
        copies[name].wait_recv()

    for load in loads:
        load.wait()
    weights = jnp.exp2(-power_ref[...].astype(F32))
    rounded = particles[...].astype(BF16)
    double = rounded.astype(F32) * (2.0 * weights)
    sources[0, 0] = double.T.astype(BF16)
    targets[0, 0, 0:HALF] = rounded[:HALF]
    targets[1, 0, 0:HALF] = rounded[HALF:]
    folded = (scores[...].astype(F32) - double).astype(BF16)
    source_scores[0, 0:ROWS] = folded[:, :W]
    target_scores[0, 0, 0:HALF] = folded[:HALF, W:]
    target_scores[1, 0, 0:HALF] = folded[HALF:, W:]

    pl.semaphore_wait(barrier, len(ids))

    def slot(step, h):
        return h if step == 1 else 8 - h

    def piece(size, step, n):
        first = 0 if step == 1 else 1
        return pl.ds((first + n) % 2 * (size // 2), size // 2)

    def z_send(kind, h, n):
        for step in (1, -1):
            src, dst = slot(step, h) % 8, slot(step, h + 1)
            if kind == "r":
                rows = piece(D, step, n)
                a, b = sources.at[src, 0, rows], sources.at[dst, 0, rows]
            else:
                rows = piece(ROWS, step, 0) if h == 3 else pl.ds(0, ROWS)
                a, b = source_scores.at[src, rows], source_scores.at[dst, rows]
            copy(("z", kind, h + 1, n, step), a, b, ("z", step))

    def to_core(kind, s):
        if kind == "r":
            copy(("core", kind, s), sources.at[s, 0], sources.at[s, 1], "core")
        else:
            block = source_scores.at[s]
            copy(("core", kind, s), block.at[pl.ds(0, ROWS)], block.at[pl.ds(ROWS, ROWS)], "core")

    def z_step(kind, h, n=0):
        for step in (1, -1):
            arrive(("z", kind, h, n, step))
        if h < 3 or (h == 3 and n == 0):
            z_send(kind, h, n)
        if n == 1 or h == 4 or kind == "s":
            for s in sorted({h, 8 - h}):
                to_core(kind, s)

    axes = (("x", "y"), ("y", "x"))

    def t_first(ref, half):
        for step, land in ((1, 3), (-1, 1)):
            copy(
                ("c1", ref is targets, half, step),
                ref.at[half, 0, pl.ds(0, HALF)],
                ref.at[half, 0, pl.ds(land * HALF, HALF)],
                (axes[half][0], step),
            )

    def t_first_far(ref, half):
        copy(
            ("c2", half),
            ref.at[half, 0, pl.ds(0, HALF)],
            ref.at[half, 0, pl.ds(2 * HALF, HALF)],
            (axes[half][0], 2),
        )

    def t_first_relay(ref, half):
        for step, src, part in ((1, 3, 0), (-1, 1, QUARTER)):
            copy(
                ("c2", half, step),
                ref.at[half, 0, pl.ds(src * HALF + part, QUARTER)],
                ref.at[half, 0, pl.ds(2 * HALF + part, QUARTER)],
                (axes[half][0], step),
            )

    def t_second(ref, half, i):
        for step, land in ((1, 3), (-1, 1)):
            copy(
                ("c3", ref is targets, half, i, step),
                ref.at[half, 0, pl.ds(i * HALF, HALF)],
                ref.at[half, land, pl.ds(i * HALF, HALF)],
                (axes[half][1], step),
            )

    def t_second_relay(ref, half, i):
        for step, src, part in ((1, 3, 0), (-1, 1, QUARTER)):
            copy(
                ("c6", ref is targets, half, i, step),
                ref.at[half, src, pl.ds(i * HALF + part, QUARTER)],
                ref.at[half, 2, pl.ds(i * HALF + part, QUARTER)],
                (axes[half][1], step),
            )

    def t_arrive(name, ref, *at):
        for half in (0, 1):
            for step in (1, -1):
                arrive((name, ref is targets, half, *at, step))

    def t_start(ref):
        for half in (0, 1):
            t_first(ref, half)
        if ref is targets:
            for half in (0, 1):
                t_first_far(ref, half)
        for half in (0, 1):
            t_second(ref, half, 0)

    def t_step1(ref):
        t_arrive("c1", ref)
        if ref is target_scores:
            for half in (0, 1):
                t_first_relay(ref, half)
        for i in (3, 1):
            for half in (0, 1):
                t_second(ref, half, i)

    def t_step2(ref):
        for half in (0, 1):
            if ref is targets:
                arrive(("c2", half))
            else:
                arrive(("c2", half, 1))
                arrive(("c2", half, -1))
        for half in (0, 1):
            t_second(ref, half, 2)

    def t_step3(ref, i):
        t_arrive("c3", ref, i)
        for half in (0, 1):
            t_second_relay(ref, half, i)

    def t_step4(ref):
        for i in range(4):
            t_arrive("c6", ref, i)

    def square_targets(tiles):
        for half, s in tiles:
            rows = targets[half, s].astype(F32)
            total = jnp.sum(rows * rows * weights, axis=1, keepdims=True) * LOG2E
            target_squares[half, s] = jnp.broadcast_to(total, (TILE, 128))

    def square_sources(s):
        for core in (0, 1):
            part = sources[s, core].astype(F32)
            total = jnp.sum(part * part * inverse[...], axis=0, keepdims=True) * LOG2E
            source_squares[s, :, core * 128 : core * 128 + 128] = total

    def make_kernels(tiles, slots):
        for tile in tiles:
            for k in slots:
                both = jnp.concatenate([sources[k, 0], sources[k, 1]], axis=1)
                inner = jnp.dot(targets[tile], both, preferred_element_type=F32)
                own = target_squares[tile]
                power = inner * LOG2E - jnp.concatenate([own, own], axis=1) - source_squares[k]
                values = jnp.exp2(power).astype(BF16)
                kernels[(*tile, k)] = values
                values = values.astype(F32)
                pair = values[:, :128] + values[:, 128:]
                if k == 0:
                    totals[tile] = pair
                else:
                    totals[tile] += pair

    def product(half, s, slots):
        left = jnp.concatenate([kernels[half, s, k] for k in slots], axis=1)
        right = jnp.concatenate([source_scores[k] for k in slots], axis=0)
        return jnp.dot(left, right, preferred_element_type=F32)

    def last_product(half, s, slots):
        row_totals = jnp.sum(totals[half, s], axis=1, keepdims=True)
        rows = targets[half, s, :, 0:W].astype(F32)
        result = product(half, s, slots) + rows * (2.0 * weights[:, :W]) * row_totals
        acc[half, s] = result
        if s == 2:
            for n, i in enumerate((2, 1, 3)):
                sent[half, s, n * HALF : n * HALF + HALF] = result[i * HALF : i * HALF + HALF].astype(BF16)
            return
        sent[half, s, 0:HALF] = result[2 * HALF : 3 * HALF].astype(BF16)
        sent[half, s, HALF : HALF + QUARTER] = result[HALF + QUARTER : 2 * HALF].astype(BF16)
        sent[half, s, HALF + QUARTER : TILE // 2] = result[3 * HALF : 3 * HALF + QUARTER].astype(BF16)

    def turn(tiles):
        for half, s in tiles:
            n = (half * 4 + s) * TILE
            turned[0:W, n : n + TILE] = target_scores[half, s].T

    def back_product(k):
        right = jnp.concatenate([kernels[half, s, k] for half in (0, 1) for s in range(4)], axis=0)
        rows = jnp.concatenate([sources[k, 0, W:], sources[k, 1, W:]], axis=1).astype(F32)
        result = jnp.dot(turned[...], right, preferred_element_type=F32)
        result = result[:W] + rows * result[W : W + 1]
        back[k] = result[:, :ROWS]
        gave[k] = result[:, ROWS:].astype(BF16)

    def give(k):
        copy(("give", k), gave.at[k], got.at[k], "core")

    def take(k):
        arrive(("give", k))
        back[k] += got[k].astype(F32)

    def back_rows(step, part):
        return pl.ds(part * ROWS if step == 1 else (1 - part) * ROWS, ROWS)

    def back_message(h, part):
        came = {(2, 0): [(4, 0), (3, 0)], (2, 1): [(3, 1)], (1, 1): [(2, 1)]}.get((h, part), [])
        for n, step in enumerate((1, -1)):
            value = back[slot(step, h), back_rows(step, part)]
            for at in came:
                arrive(("back", *at, step))
                value += back_came[(n, *at)].astype(F32)
            back_sent[n, h, part] = value.astype(BF16)

    def back_send(h, part):
        for n, step in enumerate((1, -1)):
            copy(
                ("back", h, part, step),
                back_sent.at[n, h, part],
                back_came.at[n, h, part],
                ("z", -2 * step if part == 0 and h in (2, 4) else -step),
            )

    def back_result():
        for h, part in ((1, 0), (2, 0), (1, 1)):
            for n, step in enumerate((1, -1)):
                arrive(("back", h, part, step))
                back[0, back_rows(step, part)] += back_came[n, h, part].astype(F32)
        out_ref[:, W:] = back[0].T

    def q4(n):
        return pl.ds(n * QUARTER, QUARTER)

    def first_send(half, s):
        axis = axes[half][0]
        base = sent.at[half, s]
        if s == 2:
            for n, step in enumerate((2, 1, -1)):
                rows = pl.ds(n * HALF, HALF)
                copy(("sum1", half, n), base.at[rows], arrived.at[half, s, rows], (axis, step))
            return
        copy(("rel", half, s, 1), base.at[q4(0)], relay.at[half, s, q4(0)], (axis, 1))
        copy(("rel", half, s, -1), base.at[q4(1)], relay.at[half, s, q4(1)], (axis, -1))

    def first_send_plain(half, s):
        axis = axes[half][0]
        base = sent.at[half, s]
        copy(("pln", half, s, 1), base.at[q4(2)], arrived.at[half, s, q4(1)], (axis, 1))
        copy(("pln", half, s, -1), base.at[q4(3)], arrived.at[half, s, q4(2)], (axis, -1))

    def first_add(half, s):
        for step in (1, -1):
            arrive(("rel", half, s, step))
        summed = acc[half, s, pl.ds(HALF, QUARTER)] + relay[half, s, q4(0)].astype(F32)
        sent[half, s, q4(4)] = summed.astype(BF16)
        summed = acc[half, s, pl.ds(3 * HALF + QUARTER, QUARTER)] + relay[half, s, q4(1)].astype(F32)
        sent[half, s, q4(5)] = summed.astype(BF16)

    def first_send_added(half, s):
        axis = axes[half][0]
        base = sent.at[half, s]
        copy(("add", half, s, 1), base.at[q4(4)], arrived.at[half, s, q4(0)], (axis, 1))
        copy(("add", half, s, -1), base.at[q4(5)], arrived.at[half, s, q4(3)], (axis, -1))

    def first_result(half, s):
        if s == 2:
            for n in (1, 2, 0):
                arrive(("sum1", half, n))
            came = arrived[half, s].astype(F32)
            return acc[half, s, pl.ds(0, HALF)] + came[:HALF] + came[HALF : 2 * HALF] + came[2 * HALF :]
        for name in ("pln", "add"):
            for step in (1, -1):
                arrive((name, half, s, step))
        own = acc[half, s, pl.ds(0, HALF)]
        came = arrived[half, s, 0 : 2 * HALF].astype(F32)
        return own + came[:HALF] + came[HALF:]

    def second_prepare(half, s):
        result = first_result(half, s)
        if s == 0:
            acc[half, 0, pl.ds(0, HALF)] = result
        else:
            sent2[half, s - 1] = result.astype(BF16)

    def second_send(half, s):
        copy(
            ("sum2", half, s),
            sent2.at[half, s - 1],
            arrived2.at[half, s - 1],
            (axes[half][1], (1, 2, -1)[s - 1]),
        )

    def second_result(half):
        result = acc[half, 0, pl.ds(0, HALF)]
        for s in (1, 3, 2):
            arrive(("sum2", half, s))
            result += arrived2[half, s - 1].astype(F32)
        out_ref[half * HALF : half * HALF + HALF, 0:W] = result

    near = [(0, 0), (1, 0)]
    middle = [(half, s) for s in (1, 3) for half in (0, 1)]
    far = [(0, 2), (1, 2)]
    every = near + middle + far

    def from_core(kind, slots):
        for s in slots:
            arrive(("core", kind, s))
        if kind == "r":
            for s in slots:
                square_sources(s)

    def for_both(f, *args):
        for half in (0, 1):
            f(half, *args)

    def start():
        z_send("r", 0, 0)
        t_start(targets)
        z_send("r", 0, 1)
        to_core("r", 0)
        t_start(target_scores)
        z_send("s", 0, 0)
        to_core("s", 0)
        inverse[...] = jnp.broadcast_to(0.25 / weights, (ROWS, D)).T
        turned[W:] = jnp.ones((16, 8 * TILE), BF16)

    start()
    t_step1(targets)
    z_step("r", 1, 0)
    t_step2(targets)
    z_step("r", 1, 1)
    from_core("r", (0,))
    t_step3(targets, 0)
    z_step("s", 1)
    t_step1(target_scores)
    square_targets(near)
    from_core("r", (1, 7))
    make_kernels(near, (0, 1, 7))
    z_step("r", 2, 0)
    t_step3(targets, 3)
    z_step("r", 2, 1)
    t_step3(targets, 1)
    z_step("s", 2)
    t_step3(targets, 2)
    t_step3(target_scores, 0)
    t_step2(target_scores)
    square_targets(middle)
    make_kernels(middle, (0, 1))
    z_step("r", 3, 0)
    make_kernels(middle, (7,))
    z_step("r", 3, 1)
    t_step3(target_scores, 3)
    t_step3(target_scores, 1)
    from_core("r", (2, 6))
    make_kernels(near + middle, (2, 6))
    z_step("s", 3)
    t_step3(target_scores, 2)
    t_step4(targets)
    square_targets(far)
    make_kernels(far, (0, 1, 7, 2, 6))
    z_step("r", 4)
    from_core("r", (3, 5))
    make_kernels(every, (3, 5))
    z_step("s", 4)
    from_core("r", (4,))
    make_kernels(every, (4,))
    t_step4(target_scores)
    turn(every)
    for k in (4, 3, 5):
        back_product(k)
    for k in (4, 3, 5):
        give(k)
    slots = (0, 1, 7, 2, 6, 3, 5, 4)
    from_core("s", slots)
    for s in (1, 3):
        for_both(last_product, s, slots)
    for k in (4, 3, 5):
        take(k)
    back_message(3, 1)
    back_message(4, 0)
    back_message(3, 0)
    for s in (1, 3):
        for_both(first_send, s)
    back_send(3, 1)
    back_send(4, 0)
    back_send(3, 0)
    for s in (1, 3):
        for_both(first_send_plain, s)
    for_both(last_product, 2, slots)
    for_both(first_send, 2)
    for k in (2, 6):
        back_product(k)
    for_both(last_product, 0, slots)
    for k in (2, 6):
        give(k)
    for_both(first_send, 0)
    for k in (1, 7, 0):
        back_product(k)
    for k in (1, 7, 0):
        give(k)
    for s in (1, 3):
        for_both(first_add, s)
    for s in (1, 3):
        for_both(first_send_added, s)
    for_both(first_send_plain, 0)
    take(2)
    take(6)
    back_message(2, 1)
    back_send(2, 1)
    back_message(2, 0)
    back_send(2, 0)
    for_both(first_add, 0)
    for_both(first_send_added, 0)
    for_both(second_prepare, 2)
    for_both(second_send, 2)
    for k in (1, 7, 0):
        take(k)
    back_message(1, 0)
    back_send(1, 0)
    for s in (1, 3):
        for_both(second_prepare, s)
        for_both(second_send, s)
    back_message(1, 1)
    back_send(1, 1)
    for_both(second_prepare, 0)
    for_both(second_result)
    back_result()

    for made in copies.values():
        made.wait_send()
    assert len(copies) <= COPIES


def local(particles, scores, power):
    return pl.pallas_call(
        scoped_kernel,
        out_shape=jax.ShapeDtypeStruct((ROWS, D), F32),
        in_specs=[
            pl.BlockSpec(memory_space=pltpu.HBM),
            pl.BlockSpec(memory_space=pltpu.HBM),
            pl.BlockSpec(memory_space=pltpu.HBM),
        ],
        out_specs=pl.BlockSpec(memory_space=pltpu.VMEM),
        scratch_shapes=[
            pltpu.VMEM((ROWS, D), F32),
            pltpu.VMEM((ROWS, D), BF16),
            pltpu.VMEM((1, D), jnp.int32),
            pltpu.VMEM((2, 4, TILE, D), BF16),
            pltpu.VMEM((2, 4, TILE, W), BF16),
            pltpu.VMEM((8, 2, D, ROWS), BF16),
            pltpu.VMEM((8, 2 * ROWS, W), BF16),
            pltpu.VMEM((2, 4, 8, TILE, 2 * ROWS), BF16),
            pltpu.VMEM((2, 4, TILE, W), F32),
            pltpu.VMEM((2, 4, TILE, 128), F32),
            pltpu.VMEM((8, 1, 2 * ROWS), F32),
            pltpu.VMEM((2, 4, TILE, 128), F32),
            pltpu.VMEM((D, ROWS), F32),
            pltpu.VMEM((W + 16, 8 * TILE), BF16),
            pltpu.VMEM((2, 4, 6 * QUARTER, W), BF16),
            pltpu.VMEM((2, 4, 2 * QUARTER, W), BF16),
            pltpu.VMEM((2, 4, 6 * QUARTER, W), BF16),
            pltpu.VMEM((2, 3, HALF, W), BF16),
            pltpu.VMEM((2, 3, HALF, W), BF16),
            pltpu.VMEM((8, W, ROWS), F32),
            pltpu.VMEM((8, W, ROWS), BF16),
            pltpu.VMEM((8, W, ROWS), BF16),
            pltpu.VMEM((2, 5, 2, ROWS, ROWS), BF16),
            pltpu.VMEM((2, 5, 2, ROWS, ROWS), BF16),
        ],
        compiler_params=pltpu.CompilerParams(
            collective_id=0, has_side_effects=True, vmem_limit_bytes=30 * 2**20
        ),
    )(*[pltpu.with_memory_space_constraint(a, pltpu.HBM) for a in (particles, scores, power.reshape(1, D))])


def solution(mesh):
    split = P(("gx", "gy", "gz"), None)
    return jax.shard_map(
        local, mesh=mesh, in_specs=(split, split, P()), out_specs=split, check_vma=False
    )
```

```python
import functools

import jax
import jax.numpy as jnp
from jax import lax
from jax.experimental import pallas as pl
from jax.experimental.pallas import tpu as pltpu
from jax.sharding import PartitionSpec as P

F32 = jnp.float32
BF16 = jnp.bfloat16
LOG2E = 1.4426950408889634
ROWS = 128
D = 512
W = D // 2
HALF = ROWS // 2
QUARTER = ROWS // 4
TILE = 4 * HALF
COPIES = 194


def neighbours():
    gx, gy, gz = lax.axis_index("gx"), lax.axis_index("gy"), lax.axis_index("gz")
    y_hi, x, core = gx // 8, (gx // 2) % 4, gx % 2
    y = y_hi * 2 + gz

    def at(x, y, z, core):
        return {"gx": (y // 2) * 8 + x * 2 + core, "gy": z, "gz": y % 2}

    ids = {"core": at(x, y, gy, 1 - core)}
    for step in (1, -1):
        ids["x", step] = at((x + step + 4) % 4, y, gy, core)
        ids["y", step] = at(x, (y + step + 4) % 4, gy, core)
        ids["z", step] = at(x, y, (gy + step + 8) % 8, core)
    ids["x", 2] = at((x + 2) % 4, y, gy, core)
    ids["y", 2] = at(x, (y + 2) % 4, gy, core)
    ids["z", 2] = at(x, y, (gy + 2) % 8, core)
    ids["z", -2] = at(x, y, (gy + 6) % 8, core)
    return ids


def scoped_kernel(*refs):
    pl.run_scoped(
        functools.partial(kernel, *refs),
        pltpu.SemaphoreType.DMA((3,)),
        pltpu.SemaphoreType.DMA((COPIES,)),
        pltpu.SemaphoreType.DMA((COPIES,)),
    )


def kernel(
    particles_hbm, scores_hbm, power_hbm, out_ref,
    particles, scores, power_ref, targets, target_scores, sources, source_scores, kernels, acc,
    target_squares, source_squares, totals, inverse, turned,
    sent, relay, arrived, sent2, arrived2, back, gave, got, back_sent, back_came,
    load_sem, send_sem, recv_sem,
):
    loads = [
        pltpu.make_async_copy(particles_hbm, particles, load_sem.at[0]),
        pltpu.make_async_copy(scores_hbm, scores, load_sem.at[1]),
        pltpu.make_async_copy(power_hbm, power_ref, load_sem.at[2]),
    ]
    for load in loads:
        load.start()
    ids = neighbours()
    barrier = pltpu.get_barrier_semaphore()
    for device in ids.values():
        pl.semaphore_signal(barrier, inc=1, device_id=device, device_id_type=pl.DeviceIdType.MESH)

    copies = {}

    def copy(name, src, dst, device):
        n = len(copies)
        made = pltpu.make_async_remote_copy(
            src_ref=src, dst_ref=dst, send_sem=send_sem.at[n], recv_sem=recv_sem.at[n],
            device_id=ids[device], device_id_type=pl.DeviceIdType.MESH,
        )
        assert name not in copies
        copies[name] = made
        made.start()

    def arrive(name):
        copies[name].wait_recv()

    for load in loads:
        load.wait()
    weights = jnp.exp2(-power_ref[...].astype(F32))
    rounded = particles[...].astype(BF16)
    double = rounded.astype(F32) * (2.0 * weights)
    sources[0, 0] = double.T.astype(BF16)
    targets[0, 0, 0:HALF] = rounded[:HALF]
    targets[1, 0, 0:HALF] = rounded[HALF:]
    folded = (scores[...].astype(F32) - double).astype(BF16)
    source_scores[0, 0:ROWS] = folded[:, :W]
    target_scores[0, 0, 0:HALF] = folded[:HALF, W:]
    target_scores[1, 0, 0:HALF] = folded[HALF:, W:]

    pl.semaphore_wait(barrier, len(ids))

    def slot(step, h):
        return h if step == 1 else 8 - h

    def piece(size, step, n):
        first = 0 if step == 1 else size // 2
        if n < 2:
            return pl.ds(first + n * (size // 4), size // 4)
        return pl.ds(size // 2 - first, size // 2)

    def z_send(kind, h, n):
        for step in (1, -1):
            src, dst = slot(step, h) % 8, slot(step, h + 1)
            if kind == "r":
                rows = piece(D, step, n)
                a, b = sources.at[src, 0, rows], sources.at[dst, 0, rows]
            else:
                rows = pl.ds(0 if step == 1 else HALF, HALF) if h == 3 else pl.ds(0, ROWS)
                a, b = source_scores.at[src, rows], source_scores.at[dst, rows]
            copy(("z", kind, h + 1, n, step), a, b, ("z", step))

    def to_core(kind, s):
        if kind == "r":
            copy(("core", kind, s), sources.at[s, 0], sources.at[s, 1], "core")
        else:
            block = source_scores.at[s]
            copy(("core", kind, s), block.at[pl.ds(0, ROWS)], block.at[pl.ds(ROWS, ROWS)], "core")

    def z_step(kind, h, n=0):
        for step in (1, -1):
            arrive(("z", kind, h, n, step))
        if h < 3 or (h == 3 and n < 2):
            z_send(kind, h, n)
        if n == 2 or (h == 4 and n == 1) or kind == "s":
            for s in sorted({h, 8 - h}):
                to_core(kind, s)

    axes = (("x", "y"), ("y", "x"))

    def t_first(ref, half):
        for step, land in ((1, 3), (-1, 1)):
            copy(
                ("c1", ref is targets, half, step),
                ref.at[half, 0, pl.ds(0, HALF)],
                ref.at[half, 0, pl.ds(land * HALF, HALF)],
                (axes[half][0], step),
            )

    def t_first_far(ref, half):
        copy(
            ("c2", half),
            ref.at[half, 0, pl.ds(0, HALF)],
            ref.at[half, 0, pl.ds(2 * HALF, HALF)],
            (axes[half][0], 2),
        )

    def t_first_relay(ref, half):
        for step, src, part in ((1, 3, 0), (-1, 1, QUARTER)):
            copy(
                ("c2", half, step),
                ref.at[half, 0, pl.ds(src * HALF + part, QUARTER)],
                ref.at[half, 0, pl.ds(2 * HALF + part, QUARTER)],
                (axes[half][0], step),
            )

    def t_second(ref, half, i):
        for step, land in ((1, 3), (-1, 1)):
            copy(
                ("c3", ref is targets, half, i, step),
                ref.at[half, 0, pl.ds(i * HALF, HALF)],
                ref.at[half, land, pl.ds(i * HALF, HALF)],
                (axes[half][1], step),
            )

    def t_second_relay(ref, half, i):
        for step, src, part in ((1, 3, 0), (-1, 1, QUARTER)):
            copy(
                ("c6", ref is targets, half, i, step),
                ref.at[half, src, pl.ds(i * HALF + part, QUARTER)],
                ref.at[half, 2, pl.ds(i * HALF + part, QUARTER)],
                (axes[half][1], step),
            )

    def t_arrive(name, ref, *at):
        for half in (0, 1):
            for step in (1, -1):
                arrive((name, ref is targets, half, *at, step))

    def t_start(ref):
        for half in (0, 1):
            t_first(ref, half)
        if ref is targets:
            for half in (0, 1):
                t_first_far(ref, half)
        for half in (0, 1):
            t_second(ref, half, 0)

    def t_step1(ref):
        t_arrive("c1", ref)
        if ref is target_scores:
            for half in (0, 1):
                t_first_relay(ref, half)
        for i in (3, 1):
            for half in (0, 1):
                t_second(ref, half, i)

    def t_step2(ref):
        for half in (0, 1):
            if ref is targets:
                arrive(("c2", half))
            else:
                arrive(("c2", half, 1))
                arrive(("c2", half, -1))
        for half in (0, 1):
            t_second(ref, half, 2)

    def t_step3(ref, i):
        t_arrive("c3", ref, i)
        for half in (0, 1):
            t_second_relay(ref, half, i)

    def t_step4(ref):
        for i in range(4):
            t_arrive("c6", ref, i)

    def square_targets(tiles):
        for half, s in tiles:
            rows = targets[half, s].astype(F32)
            total = jnp.sum(rows * rows * weights, axis=1, keepdims=True) * LOG2E
            target_squares[half, s] = jnp.broadcast_to(total, (TILE, 128))

    def square_sources(s):
        for core in (0, 1):
            part = sources[s, core].astype(F32)
            total = jnp.sum(part * part * inverse[...], axis=0, keepdims=True) * LOG2E
            source_squares[s, :, core * 128 : core * 128 + 128] = total

    def make_kernels(tiles, slots):
        for tile in tiles:
            for k in slots:
                both = jnp.concatenate([sources[k, 0], sources[k, 1]], axis=1)
                inner = jnp.dot(targets[tile], both, preferred_element_type=F32)
                own = target_squares[tile]
                power = inner * LOG2E - jnp.concatenate([own, own], axis=1) - source_squares[k]
                values = jnp.exp2(power).astype(BF16)
                kernels[(*tile, k)] = values
                values = values.astype(F32)
                pair = values[:, :128] + values[:, 128:]
                if k == 0:
                    totals[tile] = pair
                else:
                    totals[tile] += pair

    def product(half, s, slots):
        left = jnp.concatenate([kernels[half, s, k] for k in slots], axis=1)
        right = jnp.concatenate([source_scores[k] for k in slots], axis=0)
        return jnp.dot(left, right, preferred_element_type=F32)

    def last_product(half, s, slots):
        row_totals = jnp.sum(totals[half, s], axis=1, keepdims=True)
        rows = targets[half, s, :, 0:W].astype(F32)
        result = product(half, s, slots) + rows * (2.0 * weights[:, :W]) * row_totals
        acc[half, s] = result
        if s == 2:
            for n, i in enumerate((2, 1, 3)):
                sent[half, s, n * HALF : n * HALF + HALF] = result[i * HALF : i * HALF + HALF].astype(BF16)
            return
        sent[half, s, 0:HALF] = result[2 * HALF : 3 * HALF].astype(BF16)
        sent[half, s, HALF : HALF + QUARTER] = result[HALF + QUARTER : 2 * HALF].astype(BF16)
        sent[half, s, HALF + QUARTER : TILE // 2] = result[3 * HALF : 3 * HALF + QUARTER].astype(BF16)

    def turn(tiles):
        for half, s in tiles:
            n = (half * 4 + s) * TILE
            turned[0:W, n : n + TILE] = target_scores[half, s].T

    def back_product(k):
        right = jnp.concatenate([kernels[half, s, k] for half in (0, 1) for s in range(4)], axis=0)
        rows = jnp.concatenate([sources[k, 0, W:], sources[k, 1, W:]], axis=1).astype(F32)
        result = jnp.dot(turned[...], right, preferred_element_type=F32)
        result = result[:W] + rows * result[W : W + 1]
        back[k] = result[:, :ROWS]
        gave[k] = result[:, ROWS:].astype(BF16)

    def give(k):
        copy(("give", k), gave.at[k], got.at[k], "core")

    def take(k):
        arrive(("give", k))
        back[k] += got[k].astype(F32)

    def back_rows(step, part):
        return pl.ds(part * ROWS if step == 1 else (1 - part) * ROWS, ROWS)

    def back_message(h, part):
        came = {(2, 0): [(4, 0), (3, 0)], (2, 1): [(3, 1)], (1, 1): [(2, 1)]}.get((h, part), [])
        for n, step in enumerate((1, -1)):
            value = back[slot(step, h), back_rows(step, part)]
            for at in came:
                arrive(("back", *at, step))
                value += back_came[(n, *at)].astype(F32)
            back_sent[n, h, part] = value.astype(BF16)

    def back_send(h, part):
        for n, step in enumerate((1, -1)):
            copy(
                ("back", h, part, step),
                back_sent.at[n, h, part],
                back_came.at[n, h, part],
                ("z", -2 * step if part == 0 and h in (2, 4) else -step),
            )

    def back_result():
        for h, part in ((1, 0), (2, 0), (1, 1)):
            for n, step in enumerate((1, -1)):
                arrive(("back", h, part, step))
                back[0, back_rows(step, part)] += back_came[n, h, part].astype(F32)
        out_ref[:, W:] = back[0].T

    def q4(n):
        return pl.ds(n * QUARTER, QUARTER)

    def first_send(half, s):
        axis = axes[half][0]
        base = sent.at[half, s]
        if s == 2:
            for n, step in enumerate((2, 1, -1)):
                rows = pl.ds(n * HALF, HALF)
                copy(("sum1", half, n), base.at[rows], arrived.at[half, s, rows], (axis, step))
            return
        copy(("rel", half, s, 1), base.at[q4(0)], relay.at[half, s, q4(0)], (axis, 1))
        copy(("rel", half, s, -1), base.at[q4(1)], relay.at[half, s, q4(1)], (axis, -1))

    def first_send_plain(half, s):
        axis = axes[half][0]
        base = sent.at[half, s]
        copy(("pln", half, s, 1), base.at[q4(2)], arrived.at[half, s, q4(1)], (axis, 1))
        copy(("pln", half, s, -1), base.at[q4(3)], arrived.at[half, s, q4(2)], (axis, -1))

    def first_add(half, s):
        for step in (1, -1):
            arrive(("rel", half, s, step))
        summed = acc[half, s, pl.ds(HALF, QUARTER)] + relay[half, s, q4(0)].astype(F32)
        sent[half, s, q4(4)] = summed.astype(BF16)
        summed = acc[half, s, pl.ds(3 * HALF + QUARTER, QUARTER)] + relay[half, s, q4(1)].astype(F32)
        sent[half, s, q4(5)] = summed.astype(BF16)

    def first_send_added(half, s):
        axis = axes[half][0]
        base = sent.at[half, s]
        copy(("add", half, s, 1), base.at[q4(4)], arrived.at[half, s, q4(0)], (axis, 1))
        copy(("add", half, s, -1), base.at[q4(5)], arrived.at[half, s, q4(3)], (axis, -1))

    def first_result(half, s):
        if s == 2:
            for n in (1, 2, 0):
                arrive(("sum1", half, n))
            came = arrived[half, s].astype(F32)
            return acc[half, s, pl.ds(0, HALF)] + came[:HALF] + came[HALF : 2 * HALF] + came[2 * HALF :]
        for name in ("pln", "add"):
            for step in (1, -1):
                arrive((name, half, s, step))
        own = acc[half, s, pl.ds(0, HALF)]
        came = arrived[half, s, 0 : 2 * HALF].astype(F32)
        return own + came[:HALF] + came[HALF:]

    def second_prepare(half, s):
        result = first_result(half, s)
        if s == 0:
            acc[half, 0, pl.ds(0, HALF)] = result
        else:
            sent2[half, s - 1] = result.astype(BF16)

    def second_send(half, s):
        copy(
            ("sum2", half, s),
            sent2.at[half, s - 1],
            arrived2.at[half, s - 1],
            (axes[half][1], (1, 2, -1)[s - 1]),
        )

    def second_result(half):
        result = acc[half, 0, pl.ds(0, HALF)]
        for s in (1, 3, 2):
            arrive(("sum2", half, s))
            result += arrived2[half, s - 1].astype(F32)
        out_ref[half * HALF : half * HALF + HALF, 0:W] = result

    near = [(0, 0), (1, 0)]
    middle = [(half, s) for s in (1, 3) for half in (0, 1)]
    far = [(0, 2), (1, 2)]
    every = near + middle + far

    def from_core(kind, slots):
        for s in slots:
            arrive(("core", kind, s))
        if kind == "r":
            for s in slots:
                square_sources(s)

    def for_both(f, *args):
        for half in (0, 1):
            f(half, *args)

    def start():
        z_send("r", 0, 0)
        t_start(targets)
        z_send("r", 0, 1)
        z_send("r", 0, 2)
        to_core("r", 0)
        t_start(target_scores)
        z_send("s", 0, 0)
        to_core("s", 0)
        inverse[...] = jnp.broadcast_to(0.25 / weights, (ROWS, D)).T
        turned[W:] = jnp.ones((16, 8 * TILE), BF16)

    start()
    t_step1(targets)
    z_step("r", 1, 0)
    z_step("r", 1, 1)
    t_step2(targets)
    z_step("r", 1, 2)
    from_core("r", (0,))
    t_step3(targets, 0)
    z_step("s", 1)
    t_step1(target_scores)
    square_targets(near)
    from_core("r", (1, 7))
    make_kernels(near, (0, 1, 7))
    z_step("r", 2, 0)
    z_step("r", 2, 1)
    t_step3(targets, 3)
    z_step("r", 2, 2)
    t_step3(targets, 1)
    z_step("s", 2)
    t_step3(targets, 2)
    t_step3(target_scores, 0)
    t_step2(target_scores)
    z_step("r", 3, 0)
    square_targets(middle)
    make_kernels(middle, (0, 1))
    z_step("r", 3, 1)
    make_kernels(middle, (7,))
    z_step("r", 3, 2)
    t_step3(target_scores, 3)
    t_step3(target_scores, 1)
    from_core("r", (2, 6))
    make_kernels(near + middle, (2, 6))
    z_step("s", 3)
    t_step3(target_scores, 2)
    t_step4(targets)
    square_targets(far)
    make_kernels(far, (0, 1, 7, 2, 6))
    z_step("r", 4, 0)
    z_step("r", 4, 1)
    from_core("r", (3, 5))
    make_kernels(every, (3, 5))
    z_step("s", 4)
    from_core("r", (4,))
    make_kernels(every, (4,))
    t_step4(target_scores)
    turn(every)
    for k in (4, 3, 5):
        back_product(k)
    for k in (4, 3, 5):
        give(k)
    slots = (0, 1, 7, 2, 6, 3, 5, 4)
    from_core("s", slots)
    for s in (1, 3):
        for_both(last_product, s, slots)
    for k in (4, 3, 5):
        take(k)
    back_message(3, 1)
    back_message(4, 0)
    back_message(3, 0)
    for s in (1, 3):
        for_both(first_send, s)
    back_send(3, 1)
    back_send(4, 0)
    back_send(3, 0)
    for s in (1, 3):
        for_both(first_send_plain, s)
    for_both(last_product, 2, slots)
    for_both(first_send, 2)
    for k in (2, 6):
        back_product(k)
    for_both(last_product, 0, slots)
    for k in (2, 6):
        give(k)
    for_both(first_send, 0)
    for k in (1, 7, 0):
        back_product(k)
    for k in (1, 7, 0):
        give(k)
    for s in (1, 3):
        for_both(first_add, s)
    for s in (1, 3):
        for_both(first_send_added, s)
    for_both(first_send_plain, 0)
    take(2)
    take(6)
    back_message(2, 1)
    back_send(2, 1)
    back_message(2, 0)
    back_send(2, 0)
    for_both(first_add, 0)
    for_both(first_send_added, 0)
    for_both(second_prepare, 2)
    for_both(second_send, 2)
    for k in (1, 7, 0):
        take(k)
    back_message(1, 0)
    back_send(1, 0)
    for s in (1, 3):
        for_both(second_prepare, s)
        for_both(second_send, s)
    back_message(1, 1)
    back_send(1, 1)
    for_both(second_prepare, 0)
    for_both(second_result)
    back_result()

    for made in copies.values():
        made.wait_send()
    assert len(copies) <= COPIES


def local(particles, scores, power):
    return pl.pallas_call(
        scoped_kernel,
        out_shape=jax.ShapeDtypeStruct((ROWS, D), F32),
        in_specs=[
            pl.BlockSpec(memory_space=pltpu.HBM),
            pl.BlockSpec(memory_space=pltpu.HBM),
            pl.BlockSpec(memory_space=pltpu.HBM),
        ],
        out_specs=pl.BlockSpec(memory_space=pltpu.VMEM),
        scratch_shapes=[
            pltpu.VMEM((ROWS, D), F32),
            pltpu.VMEM((ROWS, D), BF16),
            pltpu.VMEM((1, D), jnp.int32),
            pltpu.VMEM((2, 4, TILE, D), BF16),
            pltpu.VMEM((2, 4, TILE, W), BF16),
            pltpu.VMEM((8, 2, D, ROWS), BF16),
            pltpu.VMEM((8, 2 * ROWS, W), BF16),
            pltpu.VMEM((2, 4, 8, TILE, 2 * ROWS), BF16),
            pltpu.VMEM((2, 4, TILE, W), F32),
            pltpu.VMEM((2, 4, TILE, 128), F32),
            pltpu.VMEM((8, 1, 2 * ROWS), F32),
            pltpu.VMEM((2, 4, TILE, 128), F32),
            pltpu.VMEM((D, ROWS), F32),
            pltpu.VMEM((W + 16, 8 * TILE), BF16),
            pltpu.VMEM((2, 4, 6 * QUARTER, W), BF16),
            pltpu.VMEM((2, 4, 2 * QUARTER, W), BF16),
            pltpu.VMEM((2, 4, 6 * QUARTER, W), BF16),
            pltpu.VMEM((2, 3, HALF, W), BF16),
            pltpu.VMEM((2, 3, HALF, W), BF16),
            pltpu.VMEM((8, W, ROWS), F32),
            pltpu.VMEM((8, W, ROWS), BF16),
            pltpu.VMEM((8, W, ROWS), BF16),
            pltpu.VMEM((2, 5, 2, ROWS, ROWS), BF16),
            pltpu.VMEM((2, 5, 2, ROWS, ROWS), BF16),
        ],
        compiler_params=pltpu.CompilerParams(
            collective_id=0, has_side_effects=True, vmem_limit_bytes=30 * 2**20
        ),
    )(*[pltpu.with_memory_space_constraint(a, pltpu.HBM) for a in (particles, scores, power.reshape(1, D))])


def solution(mesh):
    split = P(("gx", "gy", "gz"), None)
    return jax.shard_map(
        local, mesh=mesh, in_specs=(split, split, P()), out_specs=split, check_vma=False
    )
```

```python
import functools

import jax
import jax.numpy as jnp
from jax import lax
from jax.experimental import pallas as pl
from jax.experimental.pallas import tpu as pltpu
from jax.sharding import PartitionSpec as P

F32 = jnp.float32
BF16 = jnp.bfloat16
LOG2E = 1.4426950408889634
ROWS = 128
D = 512
W = D // 2
HALF = ROWS // 2
QUARTER = ROWS // 4
TILE = 4 * HALF
COPIES = 194


def neighbours():
    gx, gy, gz = lax.axis_index("gx"), lax.axis_index("gy"), lax.axis_index("gz")
    y_hi, x, core = gx // 8, (gx // 2) % 4, gx % 2
    y = y_hi * 2 + gz

    def at(x, y, z, core):
        return {"gx": (y // 2) * 8 + x * 2 + core, "gy": z, "gz": y % 2}

    ids = {"core": at(x, y, gy, 1 - core)}
    for step in (1, -1):
        ids["x", step] = at((x + step + 4) % 4, y, gy, core)
        ids["y", step] = at(x, (y + step + 4) % 4, gy, core)
        ids["z", step] = at(x, y, (gy + step + 8) % 8, core)
    ids["x", 2] = at((x + 2) % 4, y, gy, core)
    ids["y", 2] = at(x, (y + 2) % 4, gy, core)
    ids["z", 2] = at(x, y, (gy + 2) % 8, core)
    ids["z", -2] = at(x, y, (gy + 6) % 8, core)
    return ids


def scoped_kernel(*refs):
    pl.run_scoped(
        functools.partial(kernel, *refs),
        pltpu.SemaphoreType.DMA((3,)),
        pltpu.SemaphoreType.DMA((COPIES,)),
        pltpu.SemaphoreType.DMA((COPIES,)),
    )


def kernel(
    particles_hbm, scores_hbm, power_hbm, out_ref,
    particles, scores, power_ref, targets, target_scores, sources, source_scores, kernels, acc,
    target_squares, source_squares, totals, inverse, turned,
    sent, relay, arrived, sent2, arrived2, back, gave, got, back_sent, back_came,
    load_sem, send_sem, recv_sem,
):
    loads = [
        pltpu.make_async_copy(particles_hbm, particles, load_sem.at[0]),
        pltpu.make_async_copy(scores_hbm, scores, load_sem.at[1]),
        pltpu.make_async_copy(power_hbm, power_ref, load_sem.at[2]),
    ]
    for load in loads:
        load.start()
    ids = neighbours()
    barrier = pltpu.get_barrier_semaphore()
    for device in ids.values():
        pl.semaphore_signal(barrier, inc=1, device_id=device, device_id_type=pl.DeviceIdType.MESH)

    copies = {}

    def copy(name, src, dst, device):
        n = len(copies)
        made = pltpu.make_async_remote_copy(
            src_ref=src, dst_ref=dst, send_sem=send_sem.at[n], recv_sem=recv_sem.at[n],
            device_id=ids[device], device_id_type=pl.DeviceIdType.MESH,
        )
        assert name not in copies
        copies[name] = made
        made.start()

    def arrive(name):
        copies[name].wait_recv()

    for load in loads:
        load.wait()
    weights = jnp.exp2(-power_ref[...].astype(F32))
    rounded = particles[...].astype(BF16)
    double = rounded.astype(F32) * (2.0 * weights)
    sources[0, 0] = double.T.astype(BF16)
    targets[0, 0, 0:HALF] = rounded[:HALF]
    targets[1, 0, 0:HALF] = rounded[HALF:]

    pl.semaphore_wait(barrier, len(ids))

    def slot(step, h):
        return h if step == 1 else 8 - h

    def piece(size, step, n):
        first = 0 if step == 1 else size // 2
        if n < 2:
            return pl.ds(first + n * (size // 4), size // 4)
        return pl.ds(size // 2 - first, size // 2)

    def z_send(kind, h, n):
        for step in (1, -1):
            src, dst = slot(step, h) % 8, slot(step, h + 1)
            if kind == "r":
                rows = piece(D, step, n)
                a, b = sources.at[src, 0, rows], sources.at[dst, 0, rows]
            else:
                rows = pl.ds(0 if step == 1 else HALF, HALF) if h == 3 else pl.ds(0, ROWS)
                a, b = source_scores.at[src, rows], source_scores.at[dst, rows]
            copy(("z", kind, h + 1, n, step), a, b, ("z", step))

    def to_core(kind, s):
        if kind == "r":
            copy(("core", kind, s), sources.at[s, 0], sources.at[s, 1], "core")
        else:
            block = source_scores.at[s]
            copy(("core", kind, s), block.at[pl.ds(0, ROWS)], block.at[pl.ds(ROWS, ROWS)], "core")

    def z_step(kind, h, n=0):
        for step in (1, -1):
            arrive(("z", kind, h, n, step))
        if h < 3 or (h == 3 and n < 2):
            z_send(kind, h, n)
        if n == 2 or (h == 4 and n == 1) or kind == "s":
            for s in sorted({h, 8 - h}):
                to_core(kind, s)

    axes = (("x", "y"), ("y", "x"))

    def t_first(ref, half):
        for step, land in ((1, 3), (-1, 1)):
            copy(
                ("c1", ref is targets, half, step),
                ref.at[half, 0, pl.ds(0, HALF)],
                ref.at[half, 0, pl.ds(land * HALF, HALF)],
                (axes[half][0], step),
            )

    def t_first_far(ref, half):
        copy(
            ("c2", half),
            ref.at[half, 0, pl.ds(0, HALF)],
            ref.at[half, 0, pl.ds(2 * HALF, HALF)],
            (axes[half][0], 2),
        )

    def t_first_relay(ref, half):
        for step, src, part in ((1, 3, 0), (-1, 1, QUARTER)):
            copy(
                ("c2", half, step),
                ref.at[half, 0, pl.ds(src * HALF + part, QUARTER)],
                ref.at[half, 0, pl.ds(2 * HALF + part, QUARTER)],
                (axes[half][0], step),
            )

    def t_second(ref, half, i):
        for step, land in ((1, 3), (-1, 1)):
            copy(
                ("c3", ref is targets, half, i, step),
                ref.at[half, 0, pl.ds(i * HALF, HALF)],
                ref.at[half, land, pl.ds(i * HALF, HALF)],
                (axes[half][1], step),
            )

    def t_second_relay(ref, half, i):
        for step, src, part in ((1, 3, 0), (-1, 1, QUARTER)):
            copy(
                ("c6", ref is targets, half, i, step),
                ref.at[half, src, pl.ds(i * HALF + part, QUARTER)],
                ref.at[half, 2, pl.ds(i * HALF + part, QUARTER)],
                (axes[half][1], step),
            )

    def t_arrive(name, ref, *at):
        for half in (0, 1):
            for step in (1, -1):
                arrive((name, ref is targets, half, *at, step))

    def t_start(ref):
        for half in (0, 1):
            t_first(ref, half)
        if ref is targets:
            for half in (0, 1):
                t_first_far(ref, half)
        for half in (0, 1):
            t_second(ref, half, 0)

    def t_step1(ref):
        t_arrive("c1", ref)
        if ref is target_scores:
            for half in (0, 1):
                t_first_relay(ref, half)
        for i in (3, 1):
            for half in (0, 1):
                t_second(ref, half, i)

    def t_step2(ref):
        for half in (0, 1):
            if ref is targets:
                arrive(("c2", half))
            else:
                arrive(("c2", half, 1))
                arrive(("c2", half, -1))
        for half in (0, 1):
            t_second(ref, half, 2)

    def t_step3(ref, i):
        t_arrive("c3", ref, i)
        for half in (0, 1):
            t_second_relay(ref, half, i)

    def t_step4(ref):
        for i in range(4):
            t_arrive("c6", ref, i)

    def square_targets(tiles):
        for half, s in tiles:
            rows = targets[half, s].astype(F32)
            total = jnp.sum(rows * rows * weights, axis=1, keepdims=True) * LOG2E
            target_squares[half, s] = jnp.broadcast_to(total, (TILE, 128))

    def square_sources(s):
        for core in (0, 1):
            part = sources[s, core].astype(F32)
            total = jnp.sum(part * part * inverse[...], axis=0, keepdims=True) * LOG2E
            source_squares[s, :, core * 128 : core * 128 + 128] = total

    def make_kernels(tiles, slots):
        for tile in tiles:
            for k in slots:
                both = jnp.concatenate([sources[k, 0], sources[k, 1]], axis=1)
                inner = jnp.dot(targets[tile], both, preferred_element_type=F32)
                own = target_squares[tile]
                power = inner * LOG2E - jnp.concatenate([own, own], axis=1) - source_squares[k]
                values = jnp.exp2(power).astype(BF16)
                kernels[(*tile, k)] = values
                values = values.astype(F32)
                pair = values[:, :128] + values[:, 128:]
                if k == 0:
                    totals[tile] = pair
                else:
                    totals[tile] += pair

    def product(half, s, slots):
        left = jnp.concatenate([kernels[half, s, k] for k in slots], axis=1)
        right = jnp.concatenate([source_scores[k] for k in slots], axis=0)
        return jnp.dot(left, right, preferred_element_type=F32)

    def last_product(half, s, slots):
        row_totals = jnp.sum(totals[half, s], axis=1, keepdims=True)
        rows = targets[half, s, :, 0:W].astype(F32)
        result = product(half, s, slots) + rows * (2.0 * weights[:, :W]) * row_totals
        acc[half, s] = result
        if s == 2:
            for n, i in enumerate((2, 1, 3)):
                sent[half, s, n * HALF : n * HALF + HALF] = result[i * HALF : i * HALF + HALF].astype(BF16)
            return
        sent[half, s, 0:HALF] = result[2 * HALF : 3 * HALF].astype(BF16)
        sent[half, s, HALF : HALF + QUARTER] = result[HALF + QUARTER : 2 * HALF].astype(BF16)
        sent[half, s, HALF + QUARTER : TILE // 2] = result[3 * HALF : 3 * HALF + QUARTER].astype(BF16)

    def turn(tiles):
        for half, s in tiles:
            n = (half * 4 + s) * TILE
            turned[0:W, n : n + TILE] = target_scores[half, s].T

    def back_product(k):
        right = jnp.concatenate([kernels[half, s, k] for half in (0, 1) for s in range(4)], axis=0)
        rows = jnp.concatenate([sources[k, 0, W:], sources[k, 1, W:]], axis=1).astype(F32)
        result = jnp.dot(turned[...], right, preferred_element_type=F32)
        result = result[:W] + rows * result[W : W + 1]
        back[k] = result[:, :ROWS]
        gave[k] = result[:, ROWS:].astype(BF16)

    def give(k):
        copy(("give", k), gave.at[k], got.at[k], "core")

    def take(k):
        arrive(("give", k))
        back[k] += got[k].astype(F32)

    def back_rows(step, part):
        return pl.ds(part * ROWS if step == 1 else (1 - part) * ROWS, ROWS)

    def back_message(h, part):
        came = {(2, 0): [(4, 0), (3, 0)], (2, 1): [(3, 1)], (1, 1): [(2, 1)]}.get((h, part), [])
        for n, step in enumerate((1, -1)):
            value = back[slot(step, h), back_rows(step, part)]
            for at in came:
                arrive(("back", *at, step))
                value += back_came[(n, *at)].astype(F32)
            back_sent[n, h, part] = value.astype(BF16)

    def back_send(h, part):
        for n, step in enumerate((1, -1)):
            copy(
                ("back", h, part, step),
                back_sent.at[n, h, part],
                back_came.at[n, h, part],
                ("z", -2 * step if part == 0 and h in (2, 4) else -step),
            )

    def back_result():
        for h, part in ((1, 0), (2, 0), (1, 1)):
            for n, step in enumerate((1, -1)):
                arrive(("back", h, part, step))
                back[0, back_rows(step, part)] += back_came[n, h, part].astype(F32)
        out_ref[:, W:] = back[0].T

    def q4(n):
        return pl.ds(n * QUARTER, QUARTER)

    def first_send(half, s):
        axis = axes[half][0]
        base = sent.at[half, s]
        if s == 2:
            for n, step in enumerate((2, 1, -1)):
                rows = pl.ds(n * HALF, HALF)
                copy(("sum1", half, n), base.at[rows], arrived.at[half, s, rows], (axis, step))
            return
        copy(("rel", half, s, 1), base.at[q4(0)], relay.at[half, s, q4(0)], (axis, 1))
        copy(("rel", half, s, -1), base.at[q4(1)], relay.at[half, s, q4(1)], (axis, -1))

    def first_send_plain(half, s):
        axis = axes[half][0]
        base = sent.at[half, s]
        copy(("pln", half, s, 1), base.at[q4(2)], arrived.at[half, s, q4(1)], (axis, 1))
        copy(("pln", half, s, -1), base.at[q4(3)], arrived.at[half, s, q4(2)], (axis, -1))

    def first_add(half, s):
        for step in (1, -1):
            arrive(("rel", half, s, step))
        summed = acc[half, s, pl.ds(HALF, QUARTER)] + relay[half, s, q4(0)].astype(F32)
        sent[half, s, q4(4)] = summed.astype(BF16)
        summed = acc[half, s, pl.ds(3 * HALF + QUARTER, QUARTER)] + relay[half, s, q4(1)].astype(F32)
        sent[half, s, q4(5)] = summed.astype(BF16)

    def first_send_added(half, s):
        axis = axes[half][0]
        base = sent.at[half, s]
        copy(("add", half, s, 1), base.at[q4(4)], arrived.at[half, s, q4(0)], (axis, 1))
        copy(("add", half, s, -1), base.at[q4(5)], arrived.at[half, s, q4(3)], (axis, -1))

    def first_result(half, s):
        if s == 2:
            for n in (1, 2, 0):
                arrive(("sum1", half, n))
            came = arrived[half, s].astype(F32)
            return acc[half, s, pl.ds(0, HALF)] + came[:HALF] + came[HALF : 2 * HALF] + came[2 * HALF :]
        for name in ("pln", "add"):
            for step in (1, -1):
                arrive((name, half, s, step))
        own = acc[half, s, pl.ds(0, HALF)]
        came = arrived[half, s, 0 : 2 * HALF].astype(F32)
        return own + came[:HALF] + came[HALF:]

    def second_prepare(half, s):
        result = first_result(half, s)
        if s == 0:
            acc[half, 0, pl.ds(0, HALF)] = result
        else:
            sent2[half, s - 1] = result.astype(BF16)

    def second_send(half, s):
        copy(
            ("sum2", half, s),
            sent2.at[half, s - 1],
            arrived2.at[half, s - 1],
            (axes[half][1], (1, 2, -1)[s - 1]),
        )

    def second_result(half):
        result = acc[half, 0, pl.ds(0, HALF)]
        for s in (1, 3, 2):
            arrive(("sum2", half, s))
            result += arrived2[half, s - 1].astype(F32)
        out_ref[half * HALF : half * HALF + HALF, 0:W] = result

    near = [(0, 0), (1, 0)]
    middle = [(half, s) for s in (1, 3) for half in (0, 1)]
    far = [(0, 2), (1, 2)]
    every = near + middle + far

    def from_core(kind, slots):
        for s in slots:
            arrive(("core", kind, s))
        if kind == "r":
            for s in slots:
                square_sources(s)

    def for_both(f, *args):
        for half in (0, 1):
            f(half, *args)

    def start():
        z_send("r", 0, 0)
        t_start(targets)
        z_send("r", 0, 1)
        z_send("r", 0, 2)
        to_core("r", 0)
        folded = (scores[...].astype(F32) - double).astype(BF16)
        source_scores[0, 0:ROWS] = folded[:, :W]
        target_scores[0, 0, 0:HALF] = folded[:HALF, W:]
        target_scores[1, 0, 0:HALF] = folded[HALF:, W:]
        inverse[...] = jnp.broadcast_to(0.25 / weights, (ROWS, D)).T
        turned[W:] = jnp.ones((16, 8 * TILE), BF16)
        t_start(target_scores)
        z_send("s", 0, 0)
        to_core("s", 0)

    start()
    t_step1(targets)
    z_step("r", 1, 0)
    z_step("r", 1, 1)
    t_step2(targets)
    z_step("r", 1, 2)
    from_core("r", (0,))
    t_step3(targets, 0)
    z_step("s", 1)
    t_step1(target_scores)
    square_targets(near)
    from_core("r", (1, 7))
    make_kernels(near, (0, 1, 7))
    z_step("r", 2, 0)
    z_step("r", 2, 1)
    t_step3(targets, 3)
    z_step("r", 2, 2)
    t_step3(targets, 1)
    z_step("s", 2)
    t_step3(targets, 2)
    t_step3(target_scores, 0)
    t_step2(target_scores)
    z_step("r", 3, 0)
    square_targets(middle)
    make_kernels(middle, (0, 1))
    z_step("r", 3, 1)
    make_kernels(middle, (7,))
    z_step("r", 3, 2)
    t_step3(target_scores, 3)
    t_step3(target_scores, 1)
    from_core("r", (2, 6))
    make_kernels(near + middle, (2, 6))
    z_step("s", 3)
    t_step3(target_scores, 2)
    t_step4(targets)
    square_targets(far)
    make_kernels(far, (0, 1, 7, 2, 6))
    z_step("r", 4, 0)
    z_step("r", 4, 1)
    from_core("r", (3, 5))
    make_kernels(every, (3, 5))
    turn(near + middle)
    z_step("s", 4)
    from_core("r", (4,))
    make_kernels(every, (4,))
    t_step4(target_scores)
    turn(far)
    for k in (4, 3, 5):
        back_product(k)
    for k in (4, 3, 5):
        give(k)
    slots = (0, 1, 7, 2, 6, 3, 5, 4)
    from_core("s", slots)
    for s in (1, 3):
        for_both(last_product, s, slots)
    for k in (4, 3, 5):
        take(k)
    back_message(3, 1)
    back_message(4, 0)
    back_message(3, 0)
    for s in (1, 3):
        for_both(first_send, s)
    back_send(3, 1)
    back_send(4, 0)
    back_send(3, 0)
    for s in (1, 3):
        for_both(first_send_plain, s)
    for_both(last_product, 2, slots)
    for_both(first_send, 2)
    for k in (2, 6):
        back_product(k)
    for_both(last_product, 0, slots)
    for k in (2, 6):
        give(k)
    for_both(first_send, 0)
    for k in (1, 7, 0):
        back_product(k)
    for k in (1, 7, 0):
        give(k)
    for s in (1, 3):
        for_both(first_add, s)
    for s in (1, 3):
        for_both(first_send_added, s)
    for_both(first_send_plain, 0)
    take(2)
    take(6)
    back_message(2, 1)
    back_send(2, 1)
    back_message(2, 0)
    back_send(2, 0)
    for_both(first_add, 0)
    for_both(first_send_added, 0)
    for_both(second_prepare, 2)
    for_both(second_send, 2)
    for k in (1, 7, 0):
        take(k)
    back_message(1, 0)
    back_send(1, 0)
    for s in (1, 3):
        for_both(second_prepare, s)
        for_both(second_send, s)
    gathers = [name for name in copies if name[0] in ("z", "core", "c1", "c2", "c3", "c6", "give")]
    for name in gathers:
        copies[name].wait_send()
    back_message(1, 1)
    back_send(1, 1)
    for_both(second_prepare, 0)
    for_both(second_result)
    back_result()

    for name, made in copies.items():
        if name not in gathers:
            made.wait_send()
    assert len(copies) <= COPIES


def local(particles, scores, power):
    return pl.pallas_call(
        scoped_kernel,
        out_shape=jax.ShapeDtypeStruct((ROWS, D), F32),
        in_specs=[
            pl.BlockSpec(memory_space=pltpu.HBM),
            pl.BlockSpec(memory_space=pltpu.HBM),
            pl.BlockSpec(memory_space=pltpu.HBM),
        ],
        out_specs=pl.BlockSpec(memory_space=pltpu.VMEM),
        scratch_shapes=[
            pltpu.VMEM((ROWS, D), F32),
            pltpu.VMEM((ROWS, D), BF16),
            pltpu.VMEM((1, D), jnp.int32),
            pltpu.VMEM((2, 4, TILE, D), BF16),
            pltpu.VMEM((2, 4, TILE, W), BF16),
            pltpu.VMEM((8, 2, D, ROWS), BF16),
            pltpu.VMEM((8, 2 * ROWS, W), BF16),
            pltpu.VMEM((2, 4, 8, TILE, 2 * ROWS), BF16),
            pltpu.VMEM((2, 4, TILE, W), F32),
            pltpu.VMEM((2, 4, TILE, 128), F32),
            pltpu.VMEM((8, 1, 2 * ROWS), F32),
            pltpu.VMEM((2, 4, TILE, 128), F32),
            pltpu.VMEM((D, ROWS), F32),
            pltpu.VMEM((W + 16, 8 * TILE), BF16),
            pltpu.VMEM((2, 4, 6 * QUARTER, W), BF16),
            pltpu.VMEM((2, 4, 2 * QUARTER, W), BF16),
            pltpu.VMEM((2, 4, 6 * QUARTER, W), BF16),
            pltpu.VMEM((2, 3, HALF, W), BF16),
            pltpu.VMEM((2, 3, HALF, W), BF16),
            pltpu.VMEM((8, W, ROWS), F32),
            pltpu.VMEM((8, W, ROWS), BF16),
            pltpu.VMEM((8, W, ROWS), BF16),
            pltpu.VMEM((2, 5, 2, ROWS, ROWS), BF16),
            pltpu.VMEM((2, 5, 2, ROWS, ROWS), BF16),
        ],
        compiler_params=pltpu.CompilerParams(
            collective_id=0, has_side_effects=True, vmem_limit_bytes=30 * 2**20
        ),
    )(*[pltpu.with_memory_space_constraint(a, pltpu.HBM) for a in (particles, scores, power.reshape(1, D))])


def solution(mesh):
    split = P(("gx", "gy", "gz"), None)
    return jax.shard_map(
        local, mesh=mesh, in_specs=(split, split, P()), out_specs=split, check_vma=False
    )
```
